32 devices in a mesh: dp: 16 (over z, x, core), ens: 2 (over y).
Axes of the slice: x: 2, y: 2, z: 4, core: 2. Of those that a mesh axis runs over, the one named last changes fastest.
Arguments:
- embeddings: bfloat16 [12288, 1024], P('dp'), may hold values from -6 to 6
- valid_mask: int32 [12288], P('dp'), may hold values 0 or 1
- first_weight: bfloat16 [2, 1024, 4096], P(None, 'dp', 'ens'), may hold values from -0.1875 to 0.1875
- second_weight: bfloat16 [2, 4096, 128], P(None, 'ens'), may hold values from -0.09375 to 0.09375
- thresholds: int32 [2], replicated, may hold values from -256 to 256
Outputs:
- mean_logits: float32 [12288, 128], P('dp')
- kept_share: float32 [2], P('ens')
- agree_share: float32 [2], P('ens')
The draws below stay inside these ranges and needn't reach their ends.
All inputs are finite; a program needn't handle non-finite values. No bound on the sum of `valid_mask` on one device may be relied on, other than what follows from the above.
Results may differ from the reference program's by a relative error of at most 0.0044.
Values may be sent and summed in bfloat16 or wider, within the bound.
A program may use at most 64 MiB of HBM per device.

```python
import jax
import jax.numpy as jnp
from jax import lax

D = 1024
H = 4096
C = 128
DOC_DEV = 768
MEMBERS = 2
DOCS = 12288
N_DP = 16


def with_ends(array, stream_key, low, largest):
    index_at = [jax.random.randint(jax.random.fold_in(stream_key, axis), (), 0, length) for axis, length in enumerate(array.shape)]
    widest = array.shape.index(max(array.shape))
    next_to = index_at[:widest] + [(index_at[widest] + 1) % array.shape[widest]] + index_at[widest + 1:]
    return array.at[tuple(index_at)].set(low).at[tuple(next_to)].set(largest)


def block_scale(own_key, extent, split, least, high):
    loudness = 1.0
    for position, blocks in split:
        heights = jax.random.uniform(jax.random.fold_in(jax.random.fold_in(own_key, 6), position), (blocks,), jnp.float32, least / len(split), high / len(split))
        loudness = loudness * jnp.repeat(jnp.exp(heights), extent[position] // blocks).reshape((-1,) + (1,) * (len(extent) - 1 - position))
    return loudness


def noise(own_key, dims, scale, reach, pieces=(), kind=jnp.bfloat16):
    entries = jax.random.normal(own_key, dims, jnp.float32) * scale
    if len(pieces) > 0:
        entries = block_scale(own_key, dims, pieces, -0.22, 0.18) * entries
    return jnp.clip(entries, min=-reach, max=reach).astype(kind)


def setup_inputs(seed: int = 0) -> dict:
    seeds = jax.random.split(jax.random.key(seed), 6)
    return {
        "embeddings": noise(seeds[0], (DOCS, D), 1.0, 6.0, ((0, 16),)),
        "valid_mask": with_ends((jax.random.randint(seeds[1], (DOCS,), 0, 4) < 3).astype(jnp.int32), jax.random.fold_in(seeds[1], 1), 0, 1),
        "first_weight": noise(seeds[2], (MEMBERS, D, H), D ** -0.5, 0.1875, ((1, 16), (2, 2))),
        "second_weight": noise(seeds[3], (MEMBERS, H, C), H ** -0.5, 0.09375, ((1, 2),)),
        "thresholds": jax.random.randint(seeds[4], (MEMBERS,), -256, 257).astype(jnp.int32),
    }


def member_logits(embeddings, first_weight, second_weight):
    blocks = embeddings.reshape(N_DP, DOC_DEV, D)

    def one_member(weights):
        layer_one, layer_two = weights

        def one_block(block_rows):
            hidden = jnp.maximum(jnp.dot(block_rows, layer_one, preferred_element_type=jnp.float32), 0.0).astype(jnp.bfloat16)
            return jnp.dot(hidden, layer_two, preferred_element_type=jnp.float32)
        return lax.map(one_block, blocks).reshape(DOCS, C)
    return lax.map(one_member, (first_weight, second_weight))

def reference(embeddings, valid_mask, first_weight, second_weight, thresholds):
    logits = member_logits(embeddings, first_weight, second_weight)
    mean_logits = lax.optimization_barrier(jnp.sum(logits, axis=0)) / MEMBERS
    levels = jnp.arange(C, dtype=jnp.float32)
    grades = (2.0 * levels / (C - 1) - 1.0) * jnp.sqrt(jnp.float32(3.0 / C))
    scores = jnp.einsum('edc,c->ed', logits, grades, precision=lax.Precision.HIGHEST)
    ens_score = jnp.dot(mean_logits, grades, precision=lax.Precision.HIGHEST)
    cutoffs = thresholds.astype(jnp.float32) / 256.0
    validity = valid_mask.astype(jnp.float32)
    kept_soft = validity[None, :] * jax.nn.sigmoid(4.0 * (scores - cutoffs[:, None]))
    ens_kept = jax.nn.sigmoid(4.0 * (ens_score - jnp.mean(cutoffs)))
    kept_share = lax.optimization_barrier(jnp.sum(kept_soft, axis=1)) / DOC_DEV
    agree_share = lax.optimization_barrier(jnp.sum(kept_soft * ens_kept[None, :], axis=1)) / DOC_DEV
    return (mean_logits, kept_share, agree_share)
```

```python
import functools
import math

import jax
import jax.numpy as jnp
from jax import lax
from jax.experimental import pallas as pl
from jax.experimental.pallas import tpu as pltpu
from jax.sharding import PartitionSpec as P

MESH = pl.DeviceIdType.MESH
COLS = 256
ROWS = 256
PIECES = 4
PARTS = 4


def geometry(mesh):
    line = [tuple(d.coords) for d in mesh.devices.reshape(mesh.devices.shape[0], -1)[:, 0]]
    cores = sum(c == line[0] for c in line)
    chips = line[::cores]
    inner = 1
    if len(chips) > 1:
        axis = [a != b for a, b in zip(chips[0], chips[1])].index(True)
        while inner < len(chips) and chips[inner][axis] == chips[0][axis] + inner:
            inner += 1
    return len(chips) // inner, inner, cores


def kernel(
    geo, n_ens, emb_hbm, mask_hbm, fw_hbm, sw_hbm, thr_hbm, out_ref, share_ref,
    w, emb, sw, acc, hid, mask, thr, px_out, px_in, part, sc_out, sc_in, tot,
    local_sem, load_sem, z_send, w_recv, x_send, core_send, core_recv, doc_send, doc_recv, fwd_send,
    px_send, px_recv, part_send, part_recv, sc_send, sc_recv, tot_sem,
):
    nz, nx, nc = geo
    n_dp = nz * nx * nc
    n_chips = nz * nx
    members, rows, units = fw_hbm.shape
    chunks, width, cols = w.shape
    per_member = chunks // members
    share = units // nx
    docs, classes = out_ref.shape
    doc_part = docs // n_ens
    doc_piece = doc_part // PIECES
    step_rows = math.gcd(docs, ROWS)

    me = lax.axis_index("dp")
    ens = lax.axis_index("ens")
    core = lax.rem(me, nc)
    chip = me // nc
    z, x = chip // nx, lax.rem(chip, nx)

    def device(zz, xx, cc):
        return (zz * nx + xx) * nc + cc

    def turn(at, k, n):
        return lax.rem(at + k, n)

    def slot(xx):
        return pl.ds(pl.multiple_of(xx * docs, docs), docs)

    def origin_rows(origin):
        return pl.ds(pl.multiple_of(origin * rows, rows), rows)

    def share_cols(xx, c):
        return pl.ds(pl.multiple_of(xx * share + lax.rem(c, per_member) * cols, cols), cols)

    def own_copy(c):
        return pltpu.make_async_copy(
            fw_hbm.at[c // per_member, :, share_cols(x, c)], w.at[c, origin_rows(me), :], local_sem.at[c]
        )

    def loop(n, body):
        def step(i, carry):
            body(i)
            return carry
        lax.fori_loop(0, n, step, 0)

    loop(chunks, lambda c: own_copy(c).start())
    emb_copy = pltpu.make_async_copy(emb_hbm, emb.at[slot(x), :], load_sem.at[0])
    sw_copy = pltpu.make_async_copy(
        sw_hbm.at[:, pl.ds(pl.multiple_of(x * share, share), share), :], sw, load_sem.at[1]
    )
    mask_copy = pltpu.make_async_copy(mask_hbm, mask, load_sem.at[2])
    thr_copy = pltpu.make_async_copy(thr_hbm, thr, load_sem.at[3])

    barrier = pltpu.get_barrier_semaphore()
    waits = jnp.int32(nc - 1 + nx * n_ens - 1)
    for s in (1, -1):
        if nz > 1:
            ok = (z + s >= 0) & (z + s < nz)

            @pl.when(ok)
            def _():
                pl.semaphore_signal(barrier, inc=1, device_id={"dp": me + s * nx * nc}, device_id_type=MESH)
            waits = waits + ok.astype(jnp.int32)
    for k in range(1, nc):
        pl.semaphore_signal(
            barrier, inc=1, device_id={"dp": device(z, x, turn(core, k, nc))}, device_id_type=MESH
        )
    others = [(k, e) for k in range(nx) for e in range(n_ens) if k or e]
    for k, e in others:
        pl.semaphore_signal(
            barrier, inc=1,
            device_id={"dp": device(z, turn(x, k, nx), core), "ens": turn(ens, e, n_ens)}, device_id_type=MESH,
        )
    pl.semaphore_wait(barrier, waits)

    def block(c, zo, xo):
        return w.at[c, origin_rows(device(zo, xo, core)), :]

    def x_weights(k, c):
        xp = turn(x, k, nx)
        return pltpu.make_async_remote_copy(
            src_ref=fw_hbm.at[c // per_member, :, share_cols(xp, c)], dst_ref=w.at[c, origin_rows(me), :],
            send_sem=x_send.at[k], recv_sem=w_recv.at[z * nx + x, c],
            device_id={"dp": device(z, xp, core)}, device_id_type=MESH,
        )

    def doc_rows(xx, e, i):
        return pl.ds(pl.multiple_of(xx * docs + e * doc_part + i * doc_piece, doc_piece), doc_piece)

    def x_docs(k, i):
        xp = turn(x, k, nx)
        return pltpu.make_async_remote_copy(
            src_ref=emb_hbm.at[doc_rows(0, ens, i), :], dst_ref=emb.at[doc_rows(x, ens, i), :],
            send_sem=doc_send.at[k], recv_sem=doc_recv.at[x, ens, i],
            device_id={"dp": device(z, xp, core)}, device_id_type=MESH,
        )

    def doc_forward(k, i, e):
        xp = turn(x, k, nx)
        piece = emb.at[doc_rows(xp, ens, i), :]
        return pltpu.make_async_remote_copy(
            src_ref=piece, dst_ref=piece, send_sem=fwd_send.at[k, e], recv_sem=doc_recv.at[xp, ens, i],
            device_id={"ens": turn(ens, e, n_ens)}, device_id_type=MESH,
        )

    def doc_arrived(k, i, e):
        xp = turn(x, k, nx)
        ep = turn(ens, e, n_ens)
        piece = emb.at[doc_rows(xp, ep, i), :]
        pltpu.make_async_remote_copy(
            src_ref=piece, dst_ref=piece, send_sem=fwd_send.at[k, 0], recv_sem=doc_recv.at[xp, ep, i],
            device_id={"dp": me}, device_id_type=MESH,
        ).wait_recv()

    def z_copy(c, zo, xo, s):
        place = zo * nx + xo
        return pltpu.make_async_remote_copy(
            src_ref=block(c, zo, xo), dst_ref=block(c, zo, xo),
            send_sem=z_send.at[0 if s > 0 else 1, place], recv_sem=w_recv.at[place, c],
            device_id={"dp": me + s * nx * nc}, device_id_type=MESH,
        )

    def core_copy(c, zo, xo, k):
        return pltpu.make_async_remote_copy(
            src_ref=block(c, zo, xo), dst_ref=block(c, zo, xo),
            send_sem=core_send.at[k], recv_sem=core_recv.at[c, k],
            device_id={"dp": device(z, x, turn(core, k, nc))}, device_id_type=MESH,
        )

    def pass_on(c, zo, xo, sides):
        for s in sides:
            @pl.when((z + s >= 0) & (z + s < nz))
            def _():
                z_copy(c, zo, xo, s).start()
        for k in range(1, nc):
            core_copy(c, zo, xo, k).start()

    def arrived(c, zo, xo):
        pltpu.make_async_remote_copy(
            src_ref=block(c, zo, xo), dst_ref=block(c, zo, xo),
            send_sem=z_send.at[0, 0], recv_sem=w_recv.at[zo * nx + xo, c],
            device_id={"dp": me}, device_id_type=MESH,
        ).wait_recv()

    def from_cores(c, k):
        blocks = w.at[c, pl.ds(0, n_chips * rows), :]
        return pltpu.make_async_remote_copy(
            src_ref=blocks, dst_ref=blocks, send_sem=core_send.at[k], recv_sem=core_recv.at[c, k],
            device_id={"dp": device(z, x, turn(core, k, nc))}, device_id_type=MESH,
        )

    for k in range(1, nx):
        loop(chunks, lambda c: x_weights(k, c).start())
        for i in range(PIECES):
            x_docs(k, i).start()

    def first(c):
        own_copy(c).wait()
        pass_on(c, z, x, (1, -1))
    loop(chunks, first)
    for copy in (emb_copy, sw_copy, mask_copy, thr_copy):
        copy.start()
    acc[...] = jnp.zeros_like(acc)

    for k in range(1, nx):
        def second(c):
            arrived(c, z, turn(x, k, nx))
            pass_on(c, z, turn(x, k, nx), (1, -1))
        loop(chunks, second)

    def take(d, c):
        for s in (1, -1):
            zo = z + s * d

            @pl.when((zo >= 0) & (zo < nz))
            def _():
                for k in range(nx):
                    arrived(c, zo, turn(x, k, nx))
                    pass_on(c, zo, turn(x, k, nx), (-s,))

    def forward_docs(i):
        for k in range(1, nx):
            doc_arrived(k, i, 0)
            for e in range(1, n_ens):
                doc_forward(k, i, e).start()

    sent = 0
    for d in range(1, nz - 1):
        due = {chunks - 1: [0]} if d == 1 else {}
        if d == 2:
            for i in range(1, PIECES):
                due.setdefault((i * chunks) // (PIECES - 1) - 1, []).append(i)

        def relay(c):
            take(d, c)
            for at, pieces in due.items():
                @pl.when(c == at)
                def _():
                    for i in pieces:
                        forward_docs(i)
        loop(chunks, relay)
        sent += sum(len(v) for v in due.values())
    for i in range(sent, PIECES):
        forward_docs(i)
    for k in range(1, nx):
        for e in range(1, n_ens):
            for i in range(PIECES):
                doc_arrived(k, i, e)
    for copy in (emb_copy, sw_copy, mask_copy, thr_copy):
        copy.wait()

    def compute(c):
        for k in range(1, nc):
            from_cores(c, k).wait_recv()
        m = c // per_member
        at = pl.ds(pl.multiple_of(lax.rem(c, per_member) * cols, cols), cols)
        for r in range(0, nx * docs, step_rows):
            hid[pl.ds(r, step_rows), :] = jnp.maximum(
                jnp.dot(emb[pl.ds(r, step_rows), :], w[c], preferred_element_type=jnp.float32), 0.0
            ).astype(jnp.bfloat16)
        acc[m] += jnp.dot(hid[...], sw[m, at, :], preferred_element_type=jnp.float32)

    def last(c):
        if nz > 1:
            @pl.when(c < chunks)
            def _():
                take(nz - 1, c)

        @pl.when(c > 0)
        def _():
            compute(c - 1)
    loop(chunks + 1, last)

    lines = sc_in.shape[1]
    wide = members * classes
    lane = lax.broadcasted_iota(jnp.int32, (lines, wide), 1)
    line = lax.broadcasted_iota(jnp.int32, (lines, wide), 0)
    levels = lax.rem(lane, classes).astype(jnp.float32)
    grades = (2.0 * levels / (classes - 1) - 1.0) * jnp.sqrt(jnp.float32(3.0 / classes))
    grades = jnp.where(line == lane // classes, grades, 0.0)
    g_hi = grades.astype(jnp.bfloat16)
    g_lo = (grades - g_hi.astype(jnp.float32)).astype(jnp.bfloat16)
    g = jnp.concatenate([g_hi, g_lo], axis=0)

    def scores_of(xx):
        both = jnp.concatenate([acc[m, slot(xx), :] for m in range(members)], axis=1)
        hi = both.astype(jnp.bfloat16)
        lo = (both - hi.astype(jnp.float32)).astype(jnp.bfloat16)
        dims = (((1,), (1,)), ((), ()))
        s = lax.dot_general(g, hi, dims, preferred_element_type=jnp.float32)
        s += lax.dot_general(g, lo, dims, preferred_element_type=jnp.float32)
        return s[:lines] + s[lines:]

    mine = x * n_ens + ens

    def sc_copy(k, e):
        xp, ep = turn(x, k, nx), turn(ens, e, n_ens)
        return pltpu.make_async_remote_copy(
            src_ref=sc_out.at[k], dst_ref=sc_in.at[mine],
            send_sem=sc_send.at[k, e], recv_sem=sc_recv.at[mine],
            device_id={"dp": device(z, xp, core), "ens": ep}, device_id_type=MESH,
        )

    def sc_arrived(k, e):
        src = turn(x, k, nx) * n_ens + turn(ens, e, n_ens)
        pltpu.make_async_remote_copy(
            src_ref=sc_out.at[k], dst_ref=sc_in.at[src],
            send_sem=sc_send.at[k, e], recv_sem=sc_recv.at[src],
            device_id={"dp": me}, device_id_type=MESH,
        ).wait_recv()

    for k in list(range(1, nx)) + [0]:
        xp = turn(x, k, nx)
        s = scores_of(xp)
        sc_out[k] = s
        if k == 0:
            sc_in[mine] = s
        for e in range(n_ens):
            if k or e:
                sc_copy(k, e).start()

    def piece_of(b):
        return pl.ds(b * (docs // PARTS), docs // PARTS)

    def mean_part(xp, b):
        rows_b = pl.ds(pl.multiple_of(xp * docs + b * (docs // PARTS), docs // PARTS), docs // PARTS)
        total = acc[0, rows_b, :]
        for m in range(1, members):
            total += acc[m, rows_b, :]
        return total * (1.0 / members)

    def px_copy(k, b):
        return pltpu.make_async_remote_copy(
            src_ref=px_out.at[k, piece_of(b), :], dst_ref=px_in.at[x, piece_of(b), :],
            send_sem=px_send.at[k, b], recv_sem=px_recv.at[x, b],
            device_id={"dp": device(z, turn(x, k, nx), core)}, device_id_type=MESH,
        )

    def px_arrived(k, b):
        xp = turn(x, k, nx)
        pltpu.make_async_remote_copy(
            src_ref=px_in.at[xp, piece_of(b), :], dst_ref=px_in.at[xp, piece_of(b), :],
            send_sem=px_send.at[k, b], recv_sem=px_recv.at[xp, b],
            device_id={"dp": me}, device_id_type=MESH,
        ).wait_recv()

    def part_copy(e, b):
        piece = part.at[ens, piece_of(b), :]
        return pltpu.make_async_remote_copy(
            src_ref=piece, dst_ref=piece, send_sem=part_send.at[e, b], recv_sem=part_recv.at[ens, b],
            device_id={"ens": turn(ens, e, n_ens)}, device_id_type=MESH,
        )

    for b in range(PARTS):
        for k in range(1, nx):
            px_out[k, piece_of(b), :] = mean_part(turn(x, k, nx), b).astype(jnp.bfloat16)
            px_copy(k, b).start()

    def relay_part(b):
        total = mean_part(x, b)
        for k in range(1, nx):
            px_arrived(k, b)
            total += px_in[turn(x, k, nx), piece_of(b), :].astype(jnp.float32)
        part[ens, piece_of(b), :] = total.astype(jnp.bfloat16)
        for e in range(1, n_ens):
            part_copy(e, b).start()

    relay_part(0)
    for k, e in others:
        sc_arrived(k, e)
    scores = sc_in[0]
    for k in range(1, nx * n_ens):
        scores += sc_in[k]
    row = lax.broadcasted_iota(jnp.int32, (lines, docs), 0)
    cutoff = jnp.zeros((lines, docs), jnp.float32)
    mean_cutoff = jnp.float32(0.0)
    for m in range(members):
        level = thr[m].astype(jnp.float32) * (1.0 / 256.0)
        cutoff = jnp.where(row == m, level, cutoff)
        mean_cutoff += level * (1.0 / members)
    kept = mask[...].reshape(1, docs).astype(jnp.float32) * jax.nn.sigmoid(4.0 * (scores - cutoff))
    ens_score = jnp.sum(scores, axis=0, keepdims=True) * (1.0 / members)
    ens_kept = jax.nn.sigmoid(4.0 * (ens_score - mean_cutoff))
    kept_sum = jnp.sum(kept, axis=1, keepdims=True)
    agree_sum = jnp.sum(kept * ens_kept, axis=1, keepdims=True)
    lane = lax.broadcasted_iota(jnp.int32, (lines, 128), 1)
    tot[me] = jnp.where(lane == 0, kept_sum, jnp.where(lane == 1, agree_sum, 0.0))

    def tot_copy(k):
        return pltpu.make_async_remote_copy(
            src_ref=tot.at[me], dst_ref=tot.at[me], send_sem=tot_sem.at[0], recv_sem=tot_sem.at[1],
            device_id={"dp": lax.rem(me + k, n_dp)}, device_id_type=MESH,
        )

    tiles = tot.at[pl.ds(0, n_dp - 1)]
    all_tot = pltpu.make_async_remote_copy(
        src_ref=tiles, dst_ref=tiles, send_sem=tot_sem.at[0], recv_sem=tot_sem.at[1],
        device_id={"dp": lax.rem(me + 1, n_dp)}, device_id_type=MESH,
    )
    for k in range(1, n_dp):
        tot_copy(k).start()

    for b in range(1, PARTS):
        relay_part(b)

    for b in range(PARTS):
        for e in range(1, n_ens):
            other = turn(ens, e, n_ens)
            block_in = part.at[other, piece_of(b), :]
            pltpu.make_async_remote_copy(
                src_ref=block_in, dst_ref=block_in, send_sem=part_send.at[e, b], recv_sem=part_recv.at[other, b],
                device_id={"ens": other}, device_id_type=MESH,
            ).wait_recv()
        total = part[0, piece_of(b), :].astype(jnp.float32)
        for e in range(1, n_ens):
            total += part[e, piece_of(b), :].astype(jnp.float32)
        out_ref[piece_of(b), :] = total

    all_tot.wait_recv()
    sums = tot[0]
    for k in range(1, n_dp):
        sums += tot[k]
    sums = sums / docs
    own = members // n_ens
    row = lax.broadcasted_iota(jnp.int32, (lines, 128), 0)
    for j in range(own):
        hit = row == ens * own + j
        for i in range(2):
            share_ref[i * own + j] = jnp.sum(jnp.where(hit & (lane == i), sums, 0.0))

    for k in range(1, nx):
        whole = w.at[:, origin_rows(me), :]
        pltpu.make_async_remote_copy(
            src_ref=whole, dst_ref=whole, send_sem=x_send.at[k], recv_sem=w_recv.at[0, 0],
            device_id={"dp": device(z, turn(x, k, nx), core)}, device_id_type=MESH,
        ).wait_send()
        docs_out = emb.at[pl.ds(0, doc_part), :]
        pltpu.make_async_remote_copy(
            src_ref=docs_out, dst_ref=docs_out, send_sem=doc_send.at[k], recv_sem=doc_recv.at[0, 0, 0],
            device_id={"dp": device(z, turn(x, k, nx), core)}, device_id_type=MESH,
        ).wait_send()
        for e in range(1, n_ens):
            pltpu.make_async_remote_copy(
                src_ref=docs_out, dst_ref=docs_out, send_sem=fwd_send.at[k, e], recv_sem=doc_recv.at[0, 0, 0],
                device_id={"ens": turn(ens, e, n_ens)}, device_id_type=MESH,
            ).wait_send()
    for place in range(n_chips):
        zo, xo = divmod(place, nx)
        for s in (1, -1):
            @pl.when((z + s >= 0) & (z + s < nz) & ((zo <= z) if s > 0 else (zo >= z)))
            def _():
                whole = w.at[:, origin_rows(device(zo, xo, core)), :]
                pltpu.make_async_remote_copy(
                    src_ref=whole, dst_ref=whole,
                    send_sem=z_send.at[0 if s > 0 else 1, place], recv_sem=w_recv.at[0, 0],
                    device_id={"dp": me + s * nx * nc}, device_id_type=MESH,
                ).wait_send()
    for k in range(1, nc):
        blocks = w.at[:, pl.ds(0, n_chips * rows), :]
        pltpu.make_async_remote_copy(
            src_ref=blocks, dst_ref=blocks, send_sem=core_send.at[k], recv_sem=core_recv.at[0, k],
            device_id={"dp": device(z, x, turn(core, k, nc))}, device_id_type=MESH,
        ).wait_send()
    for k, e in others:
        sc_copy(k, e).wait_send()
    for b in range(PARTS):
        for k in range(1, nx):
            px_copy(k, b).wait_send()
        for e in range(1, n_ens):
            part_copy(e, b).wait_send()
    all_tot.wait_send()


def solution(mesh):
    geo = geometry(mesh)
    nz, nx, nc = geo
    n_dp, n_ens = mesh.shape["dp"], mesh.shape["ens"]

    def on_device(embeddings, valid_mask, first_weight, second_weight, thresholds):
        docs, width = embeddings.shape
        members, rows, units = first_weight.shape
        classes = second_weight.shape[2]
        share = units // nx
        cols = min(COLS, share)
        chunks = members * share // cols
        own = members // n_ens
        lines = -(-members // 8) * 8
        dma = pltpu.SemaphoreType.DMA
        hbm, vmem, smem = (pl.BlockSpec(memory_space=s) for s in (pl.ANY, pltpu.VMEM, pltpu.SMEM))
        mean_logits, shares = pl.pallas_call(
            functools.partial(kernel, geo, n_ens),
            out_shape=(
                pltpu.VMEM((docs, classes), jnp.float32),
                pltpu.SMEM((2 * own,), jnp.float32),
            ),
            in_specs=[hbm] * 5,
            out_specs=(vmem, smem),
            scratch_shapes=[
                pltpu.VMEM((chunks, width, cols), jnp.bfloat16),
                pltpu.VMEM((nx * docs, width), jnp.bfloat16),
                pltpu.VMEM((members, share, classes), jnp.bfloat16),
                pltpu.VMEM((members, nx * docs, classes), jnp.float32),
                pltpu.VMEM((nx * docs, cols), jnp.bfloat16),
                pltpu.VMEM(valid_mask.shape, valid_mask.dtype),
                pltpu.SMEM(thresholds.shape, thresholds.dtype),
                pltpu.VMEM((nx, docs, classes), jnp.bfloat16),
                pltpu.VMEM((nx, docs, classes), jnp.bfloat16),
                pltpu.VMEM((n_ens, docs, classes), jnp.bfloat16),
                pltpu.VMEM((nx, lines, docs), jnp.float32),
                pltpu.VMEM((nx * n_ens, lines, docs), jnp.float32),
                pltpu.VMEM((n_dp, lines, 128), jnp.float32),
                dma((chunks,)),
                dma((4,)),
                dma((2, nz * nx)),
                dma((nz * nx, chunks)),
                dma((nx,)),
                dma((nc,)),
                dma((chunks, nc)),
                dma((nx,)),
                dma((nx, n_ens, PIECES)),
                dma((nx, n_ens)),
                dma((nx, PARTS)),
                dma((nx, PARTS)),
                dma((n_ens, PARTS)),
                dma((n_ens, PARTS)),
                dma((nx, n_ens)),
                dma((nx * n_ens,)),
                dma((2,)),
            ],
            compiler_params=pltpu.CompilerParams(
                collective_id=0, has_side_effects=True, vmem_limit_bytes=63 * 1024 * 1024
            ),
        )(embeddings, valid_mask, first_weight, second_weight, thresholds)
        return mean_logits, shares[:own], shares[own:]

    return jax.shard_map(
        on_device,
        mesh=mesh,
        in_specs=(P("dp", None), P("dp"), P(None, "dp", "ens"), P(None, "ens", None), P()),
        out_specs=(P("dp", None), P("ens"), P("ens")),
        check_vma=False,
    )
```

```python
import functools
import math

import jax
import jax.numpy as jnp
from jax import lax
from jax.experimental import pallas as pl
from jax.experimental.pallas import tpu as pltpu
from jax.sharding import PartitionSpec as P

MESH = pl.DeviceIdType.MESH
COLS = 256
ROWS = 256
PIECES = 8
EARLY = 2
SPLIT = 2


def geometry(mesh):
    line = [tuple(d.coords) for d in mesh.devices.reshape(mesh.devices.shape[0], -1)[:, 0]]
    cores = sum(c == line[0] for c in line)
    chips = line[::cores]
    inner = 1
    if len(chips) > 1:
        axis = [a != b for a, b in zip(chips[0], chips[1])].index(True)
        while inner < len(chips) and chips[inner][axis] == chips[0][axis] + inner:
            inner += 1
    return len(chips) // inner, inner, cores


def kernel(
    geo, n_ens, emb_hbm, mask_hbm, fw_hbm, sw_hbm, thr_hbm, out_ref, share_ref,
    w, emb, sw, acc, hid, pre, mask, thr, px_out, px_in, part, sc_out, sc_in, tot,
    local_sem, load_sem, z_send, w_recv, x_send, core_send, core_recv, doc_send, doc_recv, fwd_send,
    px_send, px_recv, part_send, part_recv, sc_send, sc_recv, tot_sem,
):
    nz, nx, nc = geo
    n_dp = nz * nx * nc
    n_chips = nz * nx
    members, rows, units = fw_hbm.shape
    chunks, width, cols = w.shape
    per_member = chunks // members
    share = units // nx
    docs, classes = out_ref.shape
    doc_part = docs // n_ens
    pieces = doc_recv.shape[2]
    doc_piece = doc_part // pieces
    step_rows = math.gcd(docs, ROWS)
    n_blocks = docs // step_rows
    piece_rows = step_rows // SPLIT
    n_parts = docs // piece_rows
    final = chunks - 1
    plane = nx * nc * rows
    early = min(EARLY, chunks - 1)

    me = lax.axis_index("dp")
    ens = lax.axis_index("ens")
    core = lax.rem(me, nc)
    chip = me // nc
    z, x = chip // nx, lax.rem(chip, nx)
    far = jnp.where(2 * z < nz, nz - 1, 0)
    near_cols = pl.ds(pl.multiple_of(jnp.where(far == 0, plane, 0), plane), width - plane)
    far_cols = pl.ds(pl.multiple_of(far * plane, plane), plane)

    def device(zz, xx, cc):
        return (zz * nx + xx) * nc + cc

    def turn(at, k, n):
        return lax.rem(at + k, n)

    def slot(xx):
        return pl.ds(pl.multiple_of(xx * docs, docs), docs)

    def origin_rows(origin):
        return pl.ds(pl.multiple_of(origin * rows, rows), rows)

    def share_cols(xx, c):
        return pl.ds(pl.multiple_of(xx * share + lax.rem(c, per_member) * cols, cols), cols)

    def own_copy(c):
        return pltpu.make_async_copy(
            fw_hbm.at[c // per_member, :, share_cols(x, c)], w.at[c, origin_rows(me), :], local_sem.at[c]
        )

    def loop(n, body):
        def step(i, carry):
            body(i)
            return carry
        lax.fori_loop(0, n, step, 0)

    loop(chunks, lambda c: own_copy(c).start())
    emb_copy = pltpu.make_async_copy(emb_hbm, emb.at[slot(x), :], load_sem.at[0])
    sw_copy = pltpu.make_async_copy(
        sw_hbm.at[:, pl.ds(pl.multiple_of(x * share, share), share), :], sw, load_sem.at[1]
    )
    mask_copy = pltpu.make_async_copy(mask_hbm, mask, load_sem.at[2])
    thr_copy = pltpu.make_async_copy(thr_hbm, thr, load_sem.at[3])

    barrier = pltpu.get_barrier_semaphore()
    waits = jnp.int32(nc - 1 + nx * n_ens - 1)
    for s in (1, -1):
        if nz > 1:
            ok = (z + s >= 0) & (z + s < nz)

            @pl.when(ok)
            def _():
                pl.semaphore_signal(barrier, inc=1, device_id={"dp": me + s * nx * nc}, device_id_type=MESH)
            waits = waits + ok.astype(jnp.int32)
    for k in range(1, nc):
        pl.semaphore_signal(
            barrier, inc=1, device_id={"dp": device(z, x, turn(core, k, nc))}, device_id_type=MESH
        )
    others = [(k, e) for k in range(nx) for e in range(n_ens) if k or e]
    for k, e in others:
        pl.semaphore_signal(
            barrier, inc=1,
            device_id={"dp": device(z, turn(x, k, nx), core), "ens": turn(ens, e, n_ens)}, device_id_type=MESH,
        )
    pl.semaphore_wait(barrier, waits)

    def block(c, zo, xo):
        return w.at[c, origin_rows(device(zo, xo, core)), :]

    def x_weights(k, c):
        xp = turn(x, k, nx)
        return pltpu.make_async_remote_copy(
            src_ref=fw_hbm.at[c // per_member, :, share_cols(xp, c)], dst_ref=w.at[c, origin_rows(me), :],
            send_sem=x_send.at[k], recv_sem=w_recv.at[z * nx + x, c],
            device_id={"dp": device(z, xp, core)}, device_id_type=MESH,
        )

    def doc_rows(xx, e, i):
        return pl.ds(pl.multiple_of(xx * docs + e * doc_part + i * doc_piece, doc_piece), doc_piece)

    def x_docs(k, i):
        xp = turn(x, k, nx)
        return pltpu.make_async_remote_copy(
            src_ref=emb_hbm.at[doc_rows(0, ens, i), :], dst_ref=emb.at[doc_rows(x, ens, i), :],
            send_sem=doc_send.at[k], recv_sem=doc_recv.at[x, ens, i],
            device_id={"dp": device(z, xp, core)}, device_id_type=MESH,
        )

    def doc_forward(k, i, e):
        xp = turn(x, k, nx)
        piece = emb.at[doc_rows(xp, ens, i), :]
        return pltpu.make_async_remote_copy(
            src_ref=piece, dst_ref=piece, send_sem=fwd_send.at[k, e], recv_sem=doc_recv.at[xp, ens, i],
            device_id={"ens": turn(ens, e, n_ens)}, device_id_type=MESH,
        )

    def doc_arrived(k, i, e):
        xp = turn(x, k, nx)
        ep = turn(ens, e, n_ens)
        piece = emb.at[doc_rows(xp, ep, i), :]
        pltpu.make_async_remote_copy(
            src_ref=piece, dst_ref=piece, send_sem=fwd_send.at[k, 0], recv_sem=doc_recv.at[xp, ep, i],
            device_id={"dp": me}, device_id_type=MESH,
        ).wait_recv()

    def z_copy(c, zo, xo, s):
        place = zo * nx + xo
        return pltpu.make_async_remote_copy(
            src_ref=block(c, zo, xo), dst_ref=block(c, zo, xo),
            send_sem=z_send.at[0 if s > 0 else 1, place], recv_sem=w_recv.at[place, c],
            device_id={"dp": me + s * nx * nc}, device_id_type=MESH,
        )

    def core_copy(c, zo, xo, k):
        return pltpu.make_async_remote_copy(
            src_ref=block(c, zo, xo), dst_ref=block(c, zo, xo),
            send_sem=core_send.at[k], recv_sem=core_recv.at[c, k, jnp.where(zo == far, 1, 0)],
            device_id={"dp": device(z, x, turn(core, k, nc))}, device_id_type=MESH,
        )

    def pass_on(c, zo, xo, sides):
        for s in sides:
            @pl.when((z + s >= 0) & (z + s < nz))
            def _():
                z_copy(c, zo, xo, s).start()
        for k in range(1, nc):
            core_copy(c, zo, xo, k).start()

    def arrived(c, zo, xo):
        pltpu.make_async_remote_copy(
            src_ref=block(c, zo, xo), dst_ref=block(c, zo, xo),
            send_sem=z_send.at[0, 0], recv_sem=w_recv.at[zo * nx + xo, c],
            device_id={"dp": me}, device_id_type=MESH,
        ).wait_recv()

    def from_cores(c, k, is_far):
        blocks = w.at[c, pl.ds(0, (nx if is_far else n_chips - nx) * rows), :]
        return pltpu.make_async_remote_copy(
            src_ref=blocks, dst_ref=blocks, send_sem=core_send.at[k], recv_sem=core_recv.at[c, k, is_far],
            device_id={"dp": device(z, x, turn(core, k, nc))}, device_id_type=MESH,
        )

    for k in range(1, nx):
        loop(chunks, lambda c: x_weights(k, c).start())
        for i in range(pieces):
            x_docs(k, i).start()

    def first(c):
        own_copy(c).wait()
        pass_on(c, z, x, (1, -1))
    loop(chunks, first)
    for copy in (emb_copy, sw_copy, mask_copy, thr_copy):
        copy.start()
    acc[...] = jnp.zeros_like(acc)

    for k in range(1, nx):
        def second(c):
            arrived(c, z, turn(x, k, nx))
            pass_on(c, z, turn(x, k, nx), (1, -1))
        loop(chunks, second)

    def take(d, c):
        for s in (1, -1):
            zo = z + s * d

            @pl.when((zo >= 0) & (zo < nz))
            def _():
                for k in range(nx):
                    arrived(c, zo, turn(x, k, nx))
                    pass_on(c, zo, turn(x, k, nx), (-s,))

    def forward_docs(i):
        for k in range(1, nx):
            doc_arrived(k, i, 0)
            for e in range(1, n_ens):
                doc_forward(k, i, e).start()

    step_bytes = nx * rows * cols
    share_bytes = (nx - 1) * chunks * rows * cols
    due = {}
    for i in range(pieces):
        at = -(-(share_bytes + (nx - 1) * (i + 1) * doc_piece * width) // step_bytes)
        due.setdefault(min(at, (nz - 2) * chunks - 1), []).append(i)
    for d in range(1, nz - 1):
        def relay(c):
            take(d, c)
            for at, ready in due.items():
                if at // chunks == d - 1:
                    @pl.when(c == at % chunks)
                    def _():
                        for i in ready:
                            forward_docs(i)
        loop(chunks, relay)
    if nz < 3:
        for i in range(pieces):
            forward_docs(i)
    for copy in (emb_copy, sw_copy, mask_copy, thr_copy):
        copy.wait()

    def last_take(c):
        if nz > 1:
            take(nz - 1, c)

    def cores_arrived(c, sides):
        for k in range(1, nc):
            for is_far in sides:
                if is_far or nz > 1:
                    from_cores(c, k, is_far).wait_recv()

    def layer_one(c, row, into):
        hid[row, into] = jnp.maximum(
            jnp.dot(emb[row, :], w[c], preferred_element_type=jnp.float32), 0.0
        ).astype(jnp.bfloat16)

    def member_rows(c, n=1):
        m = c // per_member
        return m, pl.ds(pl.multiple_of(lax.rem(c, per_member) * cols, cols), n * cols)

    def slot_block(k, r):
        return pl.ds(pl.multiple_of(turn(x, k, nx) * docs + r * step_rows, step_rows), step_rows)

    def early_slot(k):
        for c in range(early):
            for r in range(n_blocks):
                layer_one(c, slot_block(k, r), pl.ds(c * cols, cols))
        row = slot(turn(x, k, nx))
        for c in range(early):
            m, at = member_rows(c)
            acc[m, row, :] += jnp.dot(
                hid[row, pl.ds(c * cols, cols)], sw[m, at, :], preferred_element_type=jnp.float32
            )

    def compute(c):
        cores_arrived(c, (0, 1))
        for r in range(0, nx * docs, step_rows):
            layer_one(c, pl.ds(r, step_rows), pl.ds(0, cols))
        m, at = member_rows(c)
        acc[m] += jnp.dot(hid[:, 0:cols], sw[m, at, :], preferred_element_type=jnp.float32)

    def near_slot(k):
        for r in range(n_blocks):
            row = slot_block(k, r)
            if nz > 1:
                pre[row, :] = jnp.dot(emb[row, near_cols], w[final, near_cols, :], preferred_element_type=jnp.float32)
            else:
                pre[row, :] = jnp.zeros((step_rows, cols), jnp.float32)

    def far_block(k, r):
        row = slot_block(k, r)
        total = pre[row, :] + jnp.dot(emb[row, far_cols], w[final, far_cols, :], preferred_element_type=jnp.float32)
        hid[row, 0:cols] = jnp.maximum(total, 0.0).astype(jnp.bfloat16)

    cores_arrived(final, (0,))
    near_slot(0)
    loop(early, last_take)
    for c in range(early):
        cores_arrived(c, (0, 1))
    early_slot(0)
    last_take(early)
    for k in range(1, nx):
        for e in range(1, n_ens):
            for i in range(pieces):
                doc_arrived(k, i, e)
    for k in range(1, nx):
        early_slot(k)
        near_slot(k)

    def middle(i):
        last_take(i + early + 1)
        compute(i + early)
    loop(chunks - early - 1, middle)

    cores_arrived(final, (1,))
    final_m, final_at = member_rows(final)

    def piece_of(b):
        return pl.ds(b * piece_rows, piece_rows)

    def mean_part(k, b):
        row = pl.ds(pl.multiple_of(turn(x, k, nx) * docs + b * piece_rows, piece_rows), piece_rows)
        total = acc[0, row, :]
        for m in range(1, members):
            total += acc[m, row, :]
        return total * (1.0 / members)

    def px_copy(k, b):
        return pltpu.make_async_remote_copy(
            src_ref=px_out.at[k, piece_of(b), :], dst_ref=px_in.at[x, piece_of(b), :],
            send_sem=px_send.at[k, b], recv_sem=px_recv.at[x, b],
            device_id={"dp": device(z, turn(x, k, nx), core)}, device_id_type=MESH,
        )

    for k in range(1, nx):
        for r in range(n_blocks):
            row = slot_block(k, r)
            far_block(k, r)
            acc[final_m, row, :] += jnp.dot(
                hid[row, 0:cols], sw[final_m, final_at, :], preferred_element_type=jnp.float32
            )

    lines = -(-members // 8) * 8
    wide = members * classes
    lane = lax.broadcasted_iota(jnp.int32, (lines, wide), 1)
    line = lax.broadcasted_iota(jnp.int32, (lines, wide), 0)
    levels = lax.rem(lane, classes).astype(jnp.float32)
    grades = (2.0 * levels / (classes - 1) - 1.0) * jnp.sqrt(jnp.float32(3.0 / classes))
    grades = jnp.where(line == lane // classes, grades, 0.0)
    g_hi = grades.astype(jnp.bfloat16)
    g_lo = (grades - g_hi.astype(jnp.float32)).astype(jnp.bfloat16)
    g = jnp.concatenate([g_hi, g_lo], axis=0)

    def scores_of(xx):
        both = jnp.concatenate([acc[m, slot(xx), :] for m in range(members)], axis=1)
        hi = both.astype(jnp.bfloat16)
        lo = (both - hi.astype(jnp.float32)).astype(jnp.bfloat16)
        dims = (((1,), (1,)), ((), ()))
        s = lax.dot_general(g, hi, dims, preferred_element_type=jnp.float32)
        s += lax.dot_general(g, lo, dims, preferred_element_type=jnp.float32)
        return s[:members] + s[lines : lines + members]

    mine = x * n_ens + ens

    def sc_copy(k, e):
        xp, ep = turn(x, k, nx), turn(ens, e, n_ens)
        return pltpu.make_async_remote_copy(
            src_ref=sc_out.at[k], dst_ref=sc_in.at[mine],
            send_sem=sc_send.at[k, e], recv_sem=sc_recv.at[mine],
            device_id={"dp": device(z, xp, core), "ens": ep}, device_id_type=MESH,
        )

    def sc_arrived(k, e):
        src = turn(x, k, nx) * n_ens + turn(ens, e, n_ens)
        pltpu.make_async_remote_copy(
            src_ref=sc_out.at[k], dst_ref=sc_in.at[src],
            send_sem=sc_send.at[k, e], recv_sem=sc_recv.at[src],
            device_id={"dp": me}, device_id_type=MESH,
        ).wait_recv()

    def send_scores(k):
        s = scores_of(turn(x, k, nx))
        sc_out[k] = s
        if k == 0:
            sc_in[mine] = s
        for e in range(n_ens):
            if k or e:
                sc_copy(k, e).start()

    for k in range(1, nx):
        send_scores(k)
        for b in range(n_parts):
            px_out[k, piece_of(b), :] = mean_part(k, b).astype(jnp.bfloat16)
            px_copy(k, b).start()
    for r in range(n_blocks):
        far_block(0, r)
    acc[final_m, slot(x), :] += jnp.dot(
        hid[slot(x), 0:cols], sw[final_m, final_at, :], preferred_element_type=jnp.float32
    )
    send_scores(0)

    def px_arrived(k, b):
        xp = turn(x, k, nx)
        pltpu.make_async_remote_copy(
            src_ref=px_in.at[xp, piece_of(b), :], dst_ref=px_in.at[xp, piece_of(b), :],
            send_sem=px_send.at[k, b], recv_sem=px_recv.at[xp, b],
            device_id={"dp": me}, device_id_type=MESH,
        ).wait_recv()

    def part_copy(e, b):
        piece = part.at[ens, piece_of(b), :]
        return pltpu.make_async_remote_copy(
            src_ref=piece, dst_ref=piece, send_sem=part_send.at[e, b], recv_sem=part_recv.at[ens, b],
            device_id={"ens": turn(ens, e, n_ens)}, device_id_type=MESH,
        )

    def relay_part(b):
        total = mean_part(0, b)
        for k in range(1, nx):
            px_arrived(k, b)
            total += px_in[turn(x, k, nx), piece_of(b), :].astype(jnp.float32)
        part[ens, piece_of(b), :] = total.astype(jnp.bfloat16)
        for e in range(1, n_ens):
            part_copy(e, b).start()

    for b in range(1):
        relay_part(b)
    for k, e in others:
        sc_arrived(k, e)
    scores = sc_in[0]
    for k in range(1, nx * n_ens):
        scores += sc_in[k]
    row = lax.broadcasted_iota(jnp.int32, (members, docs), 0)
    cutoff = jnp.zeros((members, docs), jnp.float32)
    mean_cutoff = jnp.float32(0.0)
    for m in range(members):
        level = thr[m].astype(jnp.float32) * (1.0 / 256.0)
        cutoff = jnp.where(row == m, level, cutoff)
        mean_cutoff += level * (1.0 / members)
    kept = mask[...].reshape(1, docs).astype(jnp.float32) * jax.nn.sigmoid(4.0 * (scores - cutoff))
    ens_score = jnp.sum(scores, axis=0, keepdims=True) * (1.0 / members)
    ens_kept = jax.nn.sigmoid(4.0 * (ens_score - mean_cutoff))
    kept_sum = jnp.sum(kept, axis=1, keepdims=True)
    agree_sum = jnp.sum(kept * ens_kept, axis=1, keepdims=True)
    lane = lax.broadcasted_iota(jnp.int32, (members, 128), 1)
    line = lax.broadcasted_iota(jnp.int32, (members, 128), 0)
    spread = jnp.where(lane == line, kept_sum, 0.0) + jnp.where(lane == line + members, agree_sum, 0.0)
    tot[me] = jnp.sum(spread, axis=0, keepdims=True)

    def tot_copy(k):
        return pltpu.make_async_remote_copy(
            src_ref=tot.at[me], dst_ref=tot.at[me], send_sem=tot_sem.at[0], recv_sem=tot_sem.at[1],
            device_id={"dp": lax.rem(me + k, n_dp)}, device_id_type=MESH,
        )

    tiles = tot.at[pl.ds(0, n_dp - 1)]
    all_tot = pltpu.make_async_remote_copy(
        src_ref=tiles, dst_ref=tiles, send_sem=tot_sem.at[0], recv_sem=tot_sem.at[1],
        device_id={"dp": lax.rem(me + 1, n_dp)}, device_id_type=MESH,
    )
    for k in range(1, n_dp):
        tot_copy(k).start()

    for b in range(1, n_parts):
        relay_part(b)

    for b in range(n_parts):
        for e in range(1, n_ens):
            other = turn(ens, e, n_ens)
            block_in = part.at[other, piece_of(b), :]
            pltpu.make_async_remote_copy(
                src_ref=block_in, dst_ref=block_in, send_sem=part_send.at[e, b], recv_sem=part_recv.at[other, b],
                device_id={"ens": other}, device_id_type=MESH,
            ).wait_recv()
        total = part[0, piece_of(b), :].astype(jnp.float32)
        for e in range(1, n_ens):
            total += part[e, piece_of(b), :].astype(jnp.float32)
        out_ref[piece_of(b), :] = total

    all_tot.wait_recv()
    sums = tot[0]
    for k in range(1, n_dp):
        sums += tot[k]
    sums = sums / docs
    own = members // n_ens
    lane = lax.broadcasted_iota(jnp.int32, sums.shape, 1)
    for j in range(own):
        for i in range(2):
            share_ref[i * own + j] = jnp.sum(jnp.where(lane == i * members + ens * own + j, sums, 0.0))

    for k in range(1, nx):
        whole = w.at[:, origin_rows(me), :]
        pltpu.make_async_remote_copy(
            src_ref=whole, dst_ref=whole, send_sem=x_send.at[k], recv_sem=w_recv.at[0, 0],
            device_id={"dp": device(z, turn(x, k, nx), core)}, device_id_type=MESH,
        ).wait_send()
        docs_out = emb.at[pl.ds(0, doc_part), :]
        pltpu.make_async_remote_copy(
            src_ref=docs_out, dst_ref=docs_out, send_sem=doc_send.at[k], recv_sem=doc_recv.at[0, 0, 0],
            device_id={"dp": device(z, turn(x, k, nx), core)}, device_id_type=MESH,
        ).wait_send()
        for e in range(1, n_ens):
            pltpu.make_async_remote_copy(
                src_ref=docs_out, dst_ref=docs_out, send_sem=fwd_send.at[k, e], recv_sem=doc_recv.at[0, 0, 0],
                device_id={"ens": turn(ens, e, n_ens)}, device_id_type=MESH,
            ).wait_send()
    for place in range(n_chips):
        zo, xo = divmod(place, nx)
        for s in (1, -1):
            @pl.when((z + s >= 0) & (z + s < nz) & ((zo <= z) if s > 0 else (zo >= z)))
            def _():
                whole = w.at[:, origin_rows(device(zo, xo, core)), :]
                pltpu.make_async_remote_copy(
                    src_ref=whole, dst_ref=whole,
                    send_sem=z_send.at[0 if s > 0 else 1, place], recv_sem=w_recv.at[0, 0],
                    device_id={"dp": me + s * nx * nc}, device_id_type=MESH,
                ).wait_send()
    for k in range(1, nc):
        blocks = w.at[:, pl.ds(0, n_chips * rows), :]
        pltpu.make_async_remote_copy(
            src_ref=blocks, dst_ref=blocks, send_sem=core_send.at[k], recv_sem=core_recv.at[0, k, 0],
            device_id={"dp": device(z, x, turn(core, k, nc))}, device_id_type=MESH,
        ).wait_send()
    for k, e in others:
        sc_copy(k, e).wait_send()
    for b in range(n_parts):
        for k in range(1, nx):
            px_copy(k, b).wait_send()
        for e in range(1, n_ens):
            part_copy(e, b).wait_send()
    all_tot.wait_send()


def solution(mesh):
    geo = geometry(mesh)
    nz, nx, nc = geo
    n_dp, n_ens = mesh.shape["dp"], mesh.shape["ens"]

    def on_device(embeddings, valid_mask, first_weight, second_weight, thresholds):
        docs, width = embeddings.shape
        members, rows, units = first_weight.shape
        classes = second_weight.shape[2]
        share = units // nx
        cols = min(COLS, share)
        chunks = members * share // cols
        own = members // n_ens
        early = min(EARLY, chunks - 1)
        parts = docs // math.gcd(docs, ROWS) * SPLIT
        pieces = math.gcd(docs // n_ens // 16, PIECES)
        dma = pltpu.SemaphoreType.DMA
        hbm, vmem, smem = (pl.BlockSpec(memory_space=s) for s in (pl.ANY, pltpu.VMEM, pltpu.SMEM))
        mean_logits, shares = pl.pallas_call(
            functools.partial(kernel, geo, n_ens),
            out_shape=(
                pltpu.VMEM((docs, classes), jnp.float32),
                pltpu.SMEM((2 * own,), jnp.float32),
            ),
            in_specs=[hbm] * 5,
            out_specs=(vmem, smem),
            scratch_shapes=[
                pltpu.VMEM((chunks, width, cols), jnp.bfloat16),
                pltpu.VMEM((nx * docs, width), jnp.bfloat16),
                pltpu.VMEM((members, share, classes), jnp.bfloat16),
                pltpu.VMEM((members, nx * docs, classes), jnp.float32),
                pltpu.VMEM((nx * docs, early * cols), jnp.bfloat16),
                pltpu.VMEM((nx * docs, cols), jnp.float32),
                pltpu.VMEM(valid_mask.shape, valid_mask.dtype),
                pltpu.SMEM(thresholds.shape, thresholds.dtype),
                pltpu.VMEM((nx, docs, classes), jnp.bfloat16),
                pltpu.VMEM((nx, docs, classes), jnp.bfloat16),
                pltpu.VMEM((n_ens, docs, classes), jnp.bfloat16),
                pltpu.VMEM((nx, members, docs), jnp.float32),
                pltpu.VMEM((nx * n_ens, members, docs), jnp.float32),
                pltpu.VMEM((n_dp, 1, 128), jnp.float32),
                dma((chunks,)),
                dma((4,)),
                dma((2, nz * nx)),
                dma((nz * nx, chunks)),
                dma((nx,)),
                dma((nc,)),
                dma((chunks, nc, 2)),
                dma((nx,)),
                dma((nx, n_ens, pieces)),
                dma((nx, n_ens)),
                dma((nx, parts)),
                dma((nx, parts)),
                dma((n_ens, parts)),
                dma((n_ens, parts)),
                dma((nx, n_ens)),
                dma((nx * n_ens,)),
                dma((2,)),
            ],
            compiler_params=pltpu.CompilerParams(
                collective_id=0, has_side_effects=True, vmem_limit_bytes=63 * 1024 * 1024
            ),
        )(embeddings, valid_mask, first_weight, second_weight, thresholds)
        return mean_logits, shares[:own], shares[own:]

    return jax.shard_map(
        on_device,
        mesh=mesh,
        in_specs=(P("dp", None), P("dp"), P(None, "dp", "ens"), P(None, "ens", None), P()),
        out_specs=(P("dp", None), P("ens"), P("ens")),
        check_vma=False,
    )
```

```python
import functools
import math

import jax
import jax.numpy as jnp
from jax import lax
from jax.experimental import pallas as pl
from jax.experimental.pallas import tpu as pltpu
from jax.sharding import PartitionSpec as P

MESH = pl.DeviceIdType.MESH
COLS = 512
ROWS = 384
PIECES = 12
EARLY = 1
SPLIT = 2
AHEAD = 1


def geometry(mesh):
    line = [tuple(d.coords) for d in mesh.devices.reshape(mesh.devices.shape[0], -1)[:, 0]]
    cores = sum(c == line[0] for c in line)
    chips = line[::cores]
    inner = 1
    if len(chips) > 1:
        axis = [a != b for a, b in zip(chips[0], chips[1])].index(True)
        while inner < len(chips) and chips[inner][axis] == chips[0][axis] + inner:
            inner += 1
    return len(chips) // inner, inner, cores


def kernel(
    geo, n_ens, emb_hbm, mask_hbm, fw_hbm, sw_hbm, thr_hbm, out_ref, share_ref,
    w, emb, sw, acc, hid, pre, mask, thr, px_out, px_in, part, sc_out, sc_in, tot,
    local_sem, load_sem, z_send, w_recv, x_send, core_send, core_recv, doc_send, doc_recv, fwd_send,
    px_send, px_recv, part_send, part_recv, sc_send, sc_recv, tot_sem,
):
    nz, nx, nc = geo
    n_dp = nz * nx * nc
    n_chips = nz * nx
    members, rows, units = fw_hbm.shape
    chunks, width, cols = w.shape
    per_member = chunks // members
    share = units // nx
    docs, classes = out_ref.shape
    doc_part = docs // n_ens
    pieces = doc_recv.shape[2]
    doc_piece = doc_part // pieces
    step_rows = math.gcd(docs, ROWS)
    n_blocks = docs // step_rows
    piece_rows = step_rows // SPLIT
    n_parts = docs // piece_rows
    final = chunks - 1
    plane = nx * nc * rows
    early = min(EARLY, chunks - 1)

    me = lax.axis_index("dp")
    ens = lax.axis_index("ens")
    core = lax.rem(me, nc)
    chip = me // nc
    z, x = chip // nx, lax.rem(chip, nx)
    inner = (z > 0) & (z < nz - 1)
    far = jnp.where(2 * z < nz, nz - 1, 0)
    near_cols = pl.ds(pl.multiple_of(jnp.where(far == 0, plane, 0), plane), width - plane)
    far_cols = pl.ds(pl.multiple_of(far * plane, plane), plane)

    def device(zz, xx, cc):
        return (zz * nx + xx) * nc + cc

    def turn(at, k, n):
        return lax.rem(at + k, n)

    def slot(xx):
        return pl.ds(pl.multiple_of(xx * docs, docs), docs)

    def origin_rows(origin):
        return pl.ds(pl.multiple_of(origin * rows, rows), rows)

    def share_cols(xx, c):
        return pl.ds(pl.multiple_of(xx * share + lax.rem(c, per_member) * cols, cols), cols)

    def own_copy(c):
        return pltpu.make_async_copy(
            fw_hbm.at[c // per_member, :, share_cols(x, c)], w.at[c, origin_rows(me), :], local_sem.at[c]
        )

    def loop(n, body):
        def step(i, carry):
            body(i)
            return carry
        lax.fori_loop(0, n, step, 0)

    loop(chunks, lambda c: own_copy(c).start())
    emb_copy = pltpu.make_async_copy(emb_hbm, emb.at[slot(x), :], load_sem.at[0])
    sw_copy = pltpu.make_async_copy(
        sw_hbm.at[:, pl.ds(pl.multiple_of(x * share, share), share), :], sw, load_sem.at[1]
    )
    mask_copy = pltpu.make_async_copy(mask_hbm, mask, load_sem.at[2])
    thr_copy = pltpu.make_async_copy(thr_hbm, thr, load_sem.at[3])

    barrier = pltpu.get_barrier_semaphore()
    waits = jnp.int32(nc - 1 + nx * n_ens - 1)
    for s in (1, -1):
        if nz > 1:
            ok = (z + s >= 0) & (z + s < nz)

            @pl.when(ok)
            def _():
                pl.semaphore_signal(barrier, inc=1, device_id={"dp": me + s * nx * nc}, device_id_type=MESH)
            waits = waits + ok.astype(jnp.int32)
    for k in range(1, nc):
        pl.semaphore_signal(
            barrier, inc=1, device_id={"dp": device(z, x, turn(core, k, nc))}, device_id_type=MESH
        )
    others = [(k, e) for k in range(nx) for e in range(n_ens) if k or e]
    for k, e in others:
        pl.semaphore_signal(
            barrier, inc=1,
            device_id={"dp": device(z, turn(x, k, nx), core), "ens": turn(ens, e, n_ens)}, device_id_type=MESH,
        )
    pl.semaphore_wait(barrier, waits)

    def block(c, zo, xo):
        return w.at[c, origin_rows(device(zo, xo, core)), :]

    def x_weights(k, c):
        xp = turn(x, k, nx)
        return pltpu.make_async_remote_copy(
            src_ref=fw_hbm.at[c // per_member, :, share_cols(xp, c)], dst_ref=w.at[c, origin_rows(me), :],
            send_sem=x_send.at[k], recv_sem=w_recv.at[z * nx + x, c],
            device_id={"dp": device(z, xp, core)}, device_id_type=MESH,
        )

    def doc_rows(xx, e, i):
        return pl.ds(pl.multiple_of(xx * docs + e * doc_part + i * doc_piece, doc_piece), doc_piece)

    def x_docs(k, i):
        xp = turn(x, k, nx)
        return pltpu.make_async_remote_copy(
            src_ref=emb_hbm.at[doc_rows(0, ens, i), :], dst_ref=emb.at[doc_rows(x, ens, i), :],
            send_sem=doc_send.at[k], recv_sem=doc_recv.at[x, ens, i],
            device_id={"dp": device(z, xp, core)}, device_id_type=MESH,
        )

    def doc_forward(k, i, e):
        xp = turn(x, k, nx)
        piece = emb.at[doc_rows(xp, ens, i), :]
        return pltpu.make_async_remote_copy(
            src_ref=piece, dst_ref=piece, send_sem=fwd_send.at[k, e], recv_sem=doc_recv.at[xp, ens, i],
            device_id={"ens": turn(ens, e, n_ens)}, device_id_type=MESH,
        )

    def doc_arrived(k, i, e):
        xp = turn(x, k, nx)
        ep = turn(ens, e, n_ens)
        piece = emb.at[doc_rows(xp, ep, i), :]
        pltpu.make_async_remote_copy(
            src_ref=piece, dst_ref=piece, send_sem=fwd_send.at[k, 0], recv_sem=doc_recv.at[xp, ep, i],
            device_id={"dp": me}, device_id_type=MESH,
        ).wait_recv()

    def z_copy(c, zo, xo, s):
        place = zo * nx + xo
        return pltpu.make_async_remote_copy(
            src_ref=block(c, zo, xo), dst_ref=block(c, zo, xo),
            send_sem=z_send.at[0 if s > 0 else 1, place], recv_sem=w_recv.at[place, c],
            device_id={"dp": me + s * nx * nc}, device_id_type=MESH,
        )

    def core_copy(c, zo, xo, k):
        return pltpu.make_async_remote_copy(
            src_ref=block(c, zo, xo), dst_ref=block(c, zo, xo),
            send_sem=core_send.at[k], recv_sem=core_recv.at[c, k, jnp.where(zo == far, 1, 0)],
            device_id={"dp": device(z, x, turn(core, k, nc))}, device_id_type=MESH,
        )

    def pass_on(c, zo, xo, sides):
        for s in sides:
            @pl.when((z + s >= 0) & (z + s < nz))
            def _():
                z_copy(c, zo, xo, s).start()
        for k in range(1, nc):
            core_copy(c, zo, xo, k).start()

    def arrived(c, zo, xo):
        pltpu.make_async_remote_copy(
            src_ref=block(c, zo, xo), dst_ref=block(c, zo, xo),
            send_sem=z_send.at[0, 0], recv_sem=w_recv.at[zo * nx + xo, c],
            device_id={"dp": me}, device_id_type=MESH,
        ).wait_recv()

    def from_cores(c, k, is_far):
        blocks = w.at[c, pl.ds(0, (nx if is_far else n_chips - nx) * rows), :]
        return pltpu.make_async_remote_copy(
            src_ref=blocks, dst_ref=blocks, send_sem=core_send.at[k], recv_sem=core_recv.at[c, k, is_far],
            device_id={"dp": device(z, x, turn(core, k, nc))}, device_id_type=MESH,
        )

    for k in range(1, nx):
        loop(chunks, lambda c: x_weights(k, c).start())
        for i in range(pieces):
            x_docs(k, i).start()

    def first(c):
        own_copy(c).wait()
        pass_on(c, z, x, (1, -1))
    loop(chunks, first)
    for copy in (emb_copy, sw_copy, mask_copy, thr_copy):
        copy.start()
    acc[...] = jnp.zeros_like(acc)

    for k in range(1, nx):
        def second(c):
            arrived(c, z, turn(x, k, nx))
            pass_on(c, z, turn(x, k, nx), (1, -1))
        loop(chunks, second)

    def take(d, c):
        for s in (1, -1):
            zo = z + s * d

            @pl.when((zo >= 0) & (zo < nz))
            def _():
                for k in range(nx):
                    arrived(c, zo, turn(x, k, nx))
                    pass_on(c, zo, turn(x, k, nx), (-s,))

    def forward_docs(i):
        for k in range(1, nx):
            doc_arrived(k, i, 0)
            for e in range(1, n_ens):
                doc_forward(k, i, e).start()

    def last_take(c):
        if nz > 1:
            take(nz - 1, c)

    def cores_arrived(c, sides):
        for k in range(1, nc):
            for is_far in sides:
                if is_far or nz > 1:
                    from_cores(c, k, is_far).wait_recv()

    def layer_one(c, row, into):
        hid[row, into] = jnp.maximum(
            jnp.dot(emb[row, :], w[c], preferred_element_type=jnp.float32), 0.0
        ).astype(jnp.bfloat16)

    def member_rows(c, n=1):
        m = c // per_member
        return m, pl.ds(pl.multiple_of(lax.rem(c, per_member) * cols, cols), n * cols)

    def slot_block(k, r):
        return pl.ds(pl.multiple_of(turn(x, k, nx) * docs + r * step_rows, step_rows), step_rows)

    def near_block(at, c, k, r):
        if nz > 1:
            row = slot_block(k, r)
            pre[at, pl.ds(r * step_rows, step_rows), :] = jnp.dot(
                emb[row, near_cols], w[c, near_cols, :], preferred_element_type=jnp.float32
            )
        else:
            pre[at, pl.ds(r * step_rows, step_rows), :] = jnp.zeros((step_rows, cols), jnp.float32)

    def near_own(c):
        cores_arrived(c, (0,))
        for r in range(n_blocks):
            near_block(c, c, 0, r)

    def far_block(at, c, k, r, into):
        row = slot_block(k, r)
        total = pre[at, pl.ds(r * step_rows, step_rows), :] + jnp.dot(
            emb[row, far_cols], w[c, far_cols, :], preferred_element_type=jnp.float32
        )
        hid[row, into] = jnp.maximum(total, 0.0).astype(jnp.bfloat16)

    def layer_two(c, k, into):
        m, at = member_rows(c)
        row = slot(turn(x, k, nx))
        acc[m, row, :] += jnp.dot(hid[row, into], sw[m, at, :], preferred_element_type=jnp.float32)

    def early_slot(k):
        for c in range(early):
            for r in range(n_blocks):
                if k == 0:
                    far_block(c, c, 0, r, pl.ds(c * cols, cols))
                else:
                    layer_one(c, slot_block(k, r), pl.ds(c * cols, cols))
        for c in range(early):
            layer_two(c, k, pl.ds(c * cols, cols))

    def own_chunk(c):
        cores_arrived(c, (1,))
        for r in range(n_blocks):
            far_block(c, c, 0, r, pl.ds(0, cols))
        layer_two(c, 0, pl.ds(0, cols))

    def compute(c):
        @pl.when(jnp.logical_not(inner))
        def _():
            cores_arrived(c, (1,))
            for k in range(nx):
                for r in range(n_blocks):
                    if k == 0:
                        far_block(c, c, 0, r, pl.ds(0, cols))
                    else:
                        layer_one(c, slot_block(k, r), pl.ds(0, cols))
            m, at = member_rows(c)
            acc[m] += jnp.dot(hid[:, 0:cols], sw[m, at, :], preferred_element_type=jnp.float32)

        @pl.when(inner)
        def _():
            for k in range(1, nx):
                for r in range(n_blocks):
                    layer_one(c, slot_block(k, r), pl.ds(0, cols))
                layer_two(c, k, pl.ds(0, cols))

    for copy in (emb_copy, sw_copy, mask_copy, thr_copy):
        copy.wait()
    step_bytes = nx * rows * cols
    share_bytes = (nx - 1) * chunks * rows * cols
    due = {}
    for i in range(pieces):
        at = -(-(share_bytes + (nx - 1) * (i + 1) * doc_piece * width) // step_bytes)
        due.setdefault(min(at, (nz - 2) * chunks - 1), []).append(i)
    for d in range(1, nz - 1):
        def relay(c):
            take(d, c)
            for at, ready in due.items():
                if at // chunks == d - 1:
                    @pl.when(c == at % chunks)
                    def _():
                        for i in ready:
                            forward_docs(i)
            if d == nz - 2:
                @pl.when(c > 0)
                def _():
                    near_own(c - 1)
        loop(chunks, relay)
    if nz < 3:
        loop(final, near_own)
        for i in range(pieces):
            forward_docs(i)
    near_own(final)
    loop(early, last_take)
    for c in range(early):
        cores_arrived(c, (1,))
    early_slot(0)
    last_take(early)

    @pl.when(inner)
    def _():
        loop(chunks - early - 1, lambda i: own_chunk(i + early))
    for k in range(1, nx):
        for e in range(1, n_ens):
            for i in range(pieces):
                doc_arrived(k, i, e)
    for k in range(1, nx):
        early_slot(k)
        for r in range(n_blocks):
            near_block(chunks + k - 1, final, k, r)

    def middle(i):
        last_take(i + early + 1)
        compute(i + early)
    loop(chunks - early - 1, middle)

    cores_arrived(final, (1,))
    final_m, final_at = member_rows(final)

    def piece_of(b):
        return pl.ds(b * piece_rows, piece_rows)

    def mean_part(k, b):
        row = pl.ds(pl.multiple_of(turn(x, k, nx) * docs + b * piece_rows, piece_rows), piece_rows)
        total = acc[0, row, :]
        for m in range(1, members):
            total += acc[m, row, :]
        return total * (1.0 / members)

    def px_copy(k, b):
        return pltpu.make_async_remote_copy(
            src_ref=px_out.at[k, piece_of(b), :], dst_ref=px_in.at[x, piece_of(b), :],
            send_sem=px_send.at[k, b], recv_sem=px_recv.at[x, b],
            device_id={"dp": device(z, turn(x, k, nx), core)}, device_id_type=MESH,
        )

    def send_parts(k, pieces_of_k):
        for b in pieces_of_k:
            px_out[k, piece_of(b), :] = mean_part(k, b).astype(jnp.bfloat16)
            px_copy(k, b).start()

    for k in range(1, nx):
        for r in range(n_blocks):
            row = slot_block(k, r)
            far_block(chunks + k - 1, final, k, r, pl.ds(0, cols))
            acc[final_m, row, :] += jnp.dot(
                hid[row, 0:cols], sw[final_m, final_at, :], preferred_element_type=jnp.float32
            )
            if r == 0:
                send_parts(k, range(AHEAD))

    lines = -(-members // 8) * 8
    wide = members * classes
    lane = lax.broadcasted_iota(jnp.int32, (lines, wide), 1)
    line = lax.broadcasted_iota(jnp.int32, (lines, wide), 0)
    levels = lax.rem(lane, classes).astype(jnp.float32)
    grades = (2.0 * levels / (classes - 1) - 1.0) * jnp.sqrt(jnp.float32(3.0 / classes))
    grades = jnp.where(line == lane // classes, grades, 0.0)
    g_hi = grades.astype(jnp.bfloat16)
    g_lo = (grades - g_hi.astype(jnp.float32)).astype(jnp.bfloat16)
    g = jnp.concatenate([g_hi, g_lo], axis=0)

    def scores_of(xx):
        both = jnp.concatenate([acc[m, slot(xx), :] for m in range(members)], axis=1)
        hi = both.astype(jnp.bfloat16)
        lo = (both - hi.astype(jnp.float32)).astype(jnp.bfloat16)
        dims = (((1,), (1,)), ((), ()))
        s = lax.dot_general(g, hi, dims, preferred_element_type=jnp.float32)
        s += lax.dot_general(g, lo, dims, preferred_element_type=jnp.float32)
        return s[:members] + s[lines : lines + members]

    mine = x * n_ens + ens

    def sc_copy(k, e):
        xp, ep = turn(x, k, nx), turn(ens, e, n_ens)
        return pltpu.make_async_remote_copy(
            src_ref=sc_out.at[k], dst_ref=sc_in.at[mine],
            send_sem=sc_send.at[k, e], recv_sem=sc_recv.at[mine],
            device_id={"dp": device(z, xp, core), "ens": ep}, device_id_type=MESH,
        )

    def sc_arrived(k, e):
        src = turn(x, k, nx) * n_ens + turn(ens, e, n_ens)
        pltpu.make_async_remote_copy(
            src_ref=sc_out.at[k], dst_ref=sc_in.at[src],
            send_sem=sc_send.at[k, e], recv_sem=sc_recv.at[src],
            device_id={"dp": me}, device_id_type=MESH,
        ).wait_recv()

    def send_scores(k):
        s = scores_of(turn(x, k, nx))
        sc_out[k] = s
        if k == 0:
            sc_in[mine] = s
        for e in range(n_ens):
            if k or e:
                sc_copy(k, e).start()

    for k in range(1, nx):
        send_scores(k)
        send_parts(k, range(AHEAD, n_parts))
    for r in range(n_blocks):
        far_block(final, final, 0, r, pl.ds(0, cols))
    acc[final_m, slot(x), :] += jnp.dot(
        hid[slot(x), 0:cols], sw[final_m, final_at, :], preferred_element_type=jnp.float32
    )
    send_scores(0)

    def px_arrived(k, b):
        xp = turn(x, k, nx)
        pltpu.make_async_remote_copy(
            src_ref=px_in.at[xp, piece_of(b), :], dst_ref=px_in.at[xp, piece_of(b), :],
            send_sem=px_send.at[k, b], recv_sem=px_recv.at[xp, b],
            device_id={"dp": me}, device_id_type=MESH,
        ).wait_recv()

    def part_copy(e, b):
        piece = part.at[ens, piece_of(b), :]
        return pltpu.make_async_remote_copy(
            src_ref=piece, dst_ref=piece, send_sem=part_send.at[e, b], recv_sem=part_recv.at[ens, b],
            device_id={"ens": turn(ens, e, n_ens)}, device_id_type=MESH,
        )

    def relay_part(b):
        total = mean_part(0, b)
        for k in range(1, nx):
            px_arrived(k, b)
            total += px_in[turn(x, k, nx), piece_of(b), :].astype(jnp.float32)
        part[ens, piece_of(b), :] = total.astype(jnp.bfloat16)
        for e in range(1, n_ens):
            part_copy(e, b).start()

    for k in range(1, nx):
        whole = w.at[:, origin_rows(me), :]
        pltpu.make_async_remote_copy(
            src_ref=whole, dst_ref=whole, send_sem=x_send.at[k], recv_sem=w_recv.at[0, 0],
            device_id={"dp": device(z, turn(x, k, nx), core)}, device_id_type=MESH,
        ).wait_send()
        docs_out = emb.at[pl.ds(0, doc_part), :]
        pltpu.make_async_remote_copy(
            src_ref=docs_out, dst_ref=docs_out, send_sem=doc_send.at[k], recv_sem=doc_recv.at[0, 0, 0],
            device_id={"dp": device(z, turn(x, k, nx), core)}, device_id_type=MESH,
        ).wait_send()
        for e in range(1, n_ens):
            pltpu.make_async_remote_copy(
                src_ref=docs_out, dst_ref=docs_out, send_sem=fwd_send.at[k, e], recv_sem=doc_recv.at[0, 0, 0],
                device_id={"ens": turn(ens, e, n_ens)}, device_id_type=MESH,
            ).wait_send()
    for place in range(n_chips):
        zo, xo = divmod(place, nx)
        for s in (1, -1):
            @pl.when((z + s >= 0) & (z + s < nz) & ((zo <= z) if s > 0 else (zo >= z)))
            def _():
                whole = w.at[:, origin_rows(device(zo, xo, core)), :]
                pltpu.make_async_remote_copy(
                    src_ref=whole, dst_ref=whole,
                    send_sem=z_send.at[0 if s > 0 else 1, place], recv_sem=w_recv.at[0, 0],
                    device_id={"dp": me + s * nx * nc}, device_id_type=MESH,
                ).wait_send()
    for k in range(1, nc):
        blocks = w.at[:, pl.ds(0, n_chips * rows), :]
        pltpu.make_async_remote_copy(
            src_ref=blocks, dst_ref=blocks, send_sem=core_send.at[k], recv_sem=core_recv.at[0, k, 0],
            device_id={"dp": device(z, x, turn(core, k, nc))}, device_id_type=MESH,
        ).wait_send()
    relay_part(0)
    for k, e in others:
        sc_arrived(k, e)
    scores = sc_in[0]
    for k in range(1, nx * n_ens):
        scores += sc_in[k]
    row = lax.broadcasted_iota(jnp.int32, (members, docs), 0)
    cutoff = jnp.zeros((members, docs), jnp.float32)
    mean_cutoff = jnp.float32(0.0)
    for m in range(members):
        level = thr[m].astype(jnp.float32) * (1.0 / 256.0)
        cutoff = jnp.where(row == m, level, cutoff)
        mean_cutoff += level * (1.0 / members)
    kept = mask[...].reshape(1, docs).astype(jnp.float32) * jax.nn.sigmoid(4.0 * (scores - cutoff))
    ens_score = jnp.sum(scores, axis=0, keepdims=True) * (1.0 / members)
    ens_kept = jax.nn.sigmoid(4.0 * (ens_score - mean_cutoff))
    kept_sum = jnp.sum(kept, axis=1, keepdims=True)
    agree_sum = jnp.sum(kept * ens_kept, axis=1, keepdims=True)
    lane = lax.broadcasted_iota(jnp.int32, (members, 128), 1)
    line = lax.broadcasted_iota(jnp.int32, (members, 128), 0)
    spread = jnp.where(lane == line, kept_sum, 0.0) + jnp.where(lane == line + members, agree_sum, 0.0)
    tot[me] = jnp.sum(spread, axis=0, keepdims=True)

    def tot_copy(k):
        return pltpu.make_async_remote_copy(
            src_ref=tot.at[me], dst_ref=tot.at[me], send_sem=tot_sem.at[0], recv_sem=tot_sem.at[1],
            device_id={"dp": lax.rem(me + k, n_dp)}, device_id_type=MESH,
        )

    tiles = tot.at[pl.ds(0, n_dp - 1)]
    all_tot = pltpu.make_async_remote_copy(
        src_ref=tiles, dst_ref=tiles, send_sem=tot_sem.at[0], recv_sem=tot_sem.at[1],
        device_id={"dp": lax.rem(me + 1, n_dp)}, device_id_type=MESH,
    )
    for k in range(1, n_dp):
        tot_copy(k).start()

    for b in range(1, n_parts):
        relay_part(b)

    for b in range(n_parts):
        for e in range(1, n_ens):
            other = turn(ens, e, n_ens)
            block_in = part.at[other, piece_of(b), :]
            pltpu.make_async_remote_copy(
                src_ref=block_in, dst_ref=block_in, send_sem=part_send.at[e, b], recv_sem=part_recv.at[other, b],
                device_id={"ens": other}, device_id_type=MESH,
            ).wait_recv()
        total = part[0, piece_of(b), :].astype(jnp.float32)
        for e in range(1, n_ens):
            total += part[e, piece_of(b), :].astype(jnp.float32)
        out_ref[piece_of(b), :] = total

    all_tot.wait_recv()
    sums = tot[0]
    for k in range(1, n_dp):
        sums += tot[k]
    sums = sums / docs
    own = members // n_ens
    lane = lax.broadcasted_iota(jnp.int32, sums.shape, 1)
    for j in range(own):
        for i in range(2):
            share_ref[i * own + j] = jnp.sum(jnp.where(lane == i * members + ens * own + j, sums, 0.0))

    for k, e in others:
        sc_copy(k, e).wait_send()
    for b in range(n_parts):
        for k in range(1, nx):
            px_copy(k, b).wait_send()
        for e in range(1, n_ens):
            part_copy(e, b).wait_send()
    all_tot.wait_send()


def solution(mesh):
    geo = geometry(mesh)
    nz, nx, nc = geo
    n_dp, n_ens = mesh.shape["dp"], mesh.shape["ens"]

    def on_device(embeddings, valid_mask, first_weight, second_weight, thresholds):
        docs, width = embeddings.shape
        members, rows, units = first_weight.shape
        classes = second_weight.shape[2]
        share = units // nx
        cols = min(COLS, share)
        chunks = members * share // cols
        own = members // n_ens
        early = min(EARLY, chunks - 1)
        parts = docs // math.gcd(docs, ROWS) * SPLIT
        pieces = math.gcd(docs // n_ens // 16, PIECES)
        dma = pltpu.SemaphoreType.DMA
        hbm, vmem, smem = (pl.BlockSpec(memory_space=s) for s in (pl.ANY, pltpu.VMEM, pltpu.SMEM))
        mean_logits, shares = pl.pallas_call(
            functools.partial(kernel, geo, n_ens),
            out_shape=(
                pltpu.VMEM((docs, classes), jnp.float32),
                pltpu.SMEM((2 * own,), jnp.float32),
            ),
            in_specs=[hbm] * 5,
            out_specs=(vmem, smem),
            scratch_shapes=[
                pltpu.VMEM((chunks, width, cols), jnp.bfloat16),
                pltpu.VMEM((nx * docs, width), jnp.bfloat16),
                pltpu.VMEM((members, share, classes), jnp.bfloat16),
                pltpu.VMEM((members, nx * docs, classes), jnp.float32),
                pltpu.VMEM((nx * docs, early * cols), jnp.bfloat16),
                pltpu.VMEM((chunks + nx - 1, docs, cols), jnp.float32),
                pltpu.VMEM(valid_mask.shape, valid_mask.dtype),
                pltpu.SMEM(thresholds.shape, thresholds.dtype),
                pltpu.VMEM((nx, docs, classes), jnp.bfloat16),
                pltpu.VMEM((nx, docs, classes), jnp.bfloat16),
                pltpu.VMEM((n_ens, docs, classes), jnp.bfloat16),
                pltpu.VMEM((nx, members, docs), jnp.float32),
                pltpu.VMEM((nx * n_ens, members, docs), jnp.float32),
                pltpu.VMEM((n_dp, 1, 128), jnp.float32),
                dma((chunks,)),
                dma((4,)),
                dma((2, nz * nx)),
                dma((nz * nx, chunks)),
                dma((nx,)),
                dma((nc,)),
                dma((chunks, nc, 2)),
                dma((nx,)),
                dma((nx, n_ens, pieces)),
                dma((nx, n_ens)),
                dma((nx, parts)),
                dma((nx, parts)),
                dma((n_ens, parts)),
                dma((n_ens, parts)),
                dma((nx, n_ens)),
                dma((nx * n_ens,)),
                dma((2,)),
            ],
            compiler_params=pltpu.CompilerParams(
                collective_id=0, has_side_effects=True, vmem_limit_bytes=63 * 1024 * 1024
            ),
        )(embeddings, valid_mask, first_weight, second_weight, thresholds)
        return mean_logits, shares[:own], shares[own:]

    return jax.shard_map(
        on_device,
        mesh=mesh,
        in_specs=(P("dp", None), P("dp"), P(None, "dp", "ens"), P(None, "ens", None), P()),
        out_specs=(P("dp", None), P("ens"), P("ens")),
        check_vma=False,
    )
```

```python
import functools
import math

import jax
import jax.numpy as jnp
from jax import lax
from jax.experimental import pallas as pl
from jax.experimental.pallas import tpu as pltpu
from jax.sharding import PartitionSpec as P

MESH = pl.DeviceIdType.MESH
COLS = 512
ROWS = 384
PIECES = 12
EARLY = 1
SPLIT = 3
AHEAD = 1


def geometry(mesh):
    line = [tuple(d.coords) for d in mesh.devices.reshape(mesh.devices.shape[0], -1)[:, 0]]
    cores = sum(c == line[0] for c in line)
    chips = line[::cores]
    inner = 1
    if len(chips) > 1:
        axis = [a != b for a, b in zip(chips[0], chips[1])].index(True)
        while inner < len(chips) and chips[inner][axis] == chips[0][axis] + inner:
            inner += 1
    return len(chips) // inner, inner, cores


def kernel(
    geo, n_ens, emb_hbm, mask_hbm, fw_hbm, sw_hbm, thr_hbm, out_ref, share_ref,
    w, emb, sw, acc, hid, pre, mask, thr, px_out, px_in, part, sc_out, sc_in, tot,
    local_sem, load_sem, z_send, w_recv, x_send, core_send, core_recv, doc_send, doc_recv, fwd_send,
    px_send, px_recv, part_send, part_recv, sc_send, sc_recv, tot_sem,
):
    nz, nx, nc = geo
    n_dp = nz * nx * nc
    n_chips = nz * nx
    members, rows, units = fw_hbm.shape
    chunks, width, cols = w.shape
    per_member = chunks // members
    share = units // nx
    docs, classes = out_ref.shape
    doc_part = docs // n_ens
    pieces = doc_recv.shape[2]
    doc_piece = doc_part // pieces
    step_rows = math.gcd(docs, ROWS)
    n_blocks = docs // step_rows
    piece_rows = step_rows // SPLIT
    n_parts = docs // piece_rows
    final = chunks - 1
    plane = nx * nc * rows
    early = min(EARLY, chunks - 1)

    me = lax.axis_index("dp")
    ens = lax.axis_index("ens")
    core = lax.rem(me, nc)
    chip = me // nc
    z, x = chip // nx, lax.rem(chip, nx)
    inner = (z > 0) & (z < nz - 1)
    far = jnp.where(2 * z < nz, nz - 1, 0)
    near_cols = pl.ds(pl.multiple_of(jnp.where(far == 0, plane, 0), plane), width - plane)
    far_cols = pl.ds(pl.multiple_of(far * plane, plane), plane)

    def device(zz, xx, cc):
        return (zz * nx + xx) * nc + cc

    def turn(at, k, n):
        return lax.rem(at + k, n)

    def slot(xx):
        return pl.ds(pl.multiple_of(xx * docs, docs), docs)

    def origin_rows(origin):
        return pl.ds(pl.multiple_of(origin * rows, rows), rows)

    def share_cols(xx, c):
        return pl.ds(pl.multiple_of(xx * share + lax.rem(c, per_member) * cols, cols), cols)

    def own_copy(c):
        return pltpu.make_async_copy(
            fw_hbm.at[c // per_member, :, share_cols(x, c)], w.at[c, origin_rows(me), :], local_sem.at[c]
        )

    def loop(n, body):
        def step(i, carry):
            body(i)
            return carry
        lax.fori_loop(0, n, step, 0)

    loop(chunks, lambda c: own_copy(c).start())
    emb_copy = pltpu.make_async_copy(emb_hbm, emb.at[slot(x), :], load_sem.at[0])
    sw_copy = pltpu.make_async_copy(
        sw_hbm.at[:, pl.ds(pl.multiple_of(x * share, share), share), :], sw, load_sem.at[1]
    )
    mask_copy = pltpu.make_async_copy(mask_hbm, mask, load_sem.at[2])
    thr_copy = pltpu.make_async_copy(thr_hbm, thr, load_sem.at[3])

    barrier = pltpu.get_barrier_semaphore()
    waits = jnp.int32(nc - 1 + nx * n_ens - 1)
    for s in (1, -1):
        if nz > 1:
            ok = (z + s >= 0) & (z + s < nz)

            @pl.when(ok)
            def _():
                pl.semaphore_signal(barrier, inc=1, device_id={"dp": me + s * nx * nc}, device_id_type=MESH)
            waits = waits + ok.astype(jnp.int32)
    for k in range(1, nc):
        pl.semaphore_signal(
            barrier, inc=1, device_id={"dp": device(z, x, turn(core, k, nc))}, device_id_type=MESH
        )
    others = [(k, e) for k in range(nx) for e in range(n_ens) if k or e]
    for k, e in others:
        pl.semaphore_signal(
            barrier, inc=1,
            device_id={"dp": device(z, turn(x, k, nx), core), "ens": turn(ens, e, n_ens)}, device_id_type=MESH,
        )
    pl.semaphore_wait(barrier, waits)

    def block(c, zo, xo):
        return w.at[c, origin_rows(device(zo, xo, core)), :]

    def x_weights(k, c):
        xp = turn(x, k, nx)
        return pltpu.make_async_remote_copy(
            src_ref=fw_hbm.at[c // per_member, :, share_cols(xp, c)], dst_ref=w.at[c, origin_rows(me), :],
            send_sem=x_send.at[k], recv_sem=w_recv.at[z * nx + x, c],
            device_id={"dp": device(z, xp, core)}, device_id_type=MESH,
        )

    def doc_rows(xx, e, i):
        return pl.ds(pl.multiple_of(xx * docs + e * doc_part + i * doc_piece, doc_piece), doc_piece)

    def x_docs(k, i):
        xp = turn(x, k, nx)
        return pltpu.make_async_remote_copy(
            src_ref=emb_hbm.at[doc_rows(0, ens, i), :], dst_ref=emb.at[doc_rows(x, ens, i), :],
            send_sem=doc_send.at[k], recv_sem=doc_recv.at[x, ens, i],
            device_id={"dp": device(z, xp, core)}, device_id_type=MESH,
        )

    def doc_forward(k, i, e):
        xp = turn(x, k, nx)
        piece = emb.at[doc_rows(xp, ens, i), :]
        return pltpu.make_async_remote_copy(
            src_ref=piece, dst_ref=piece, send_sem=fwd_send.at[k, e], recv_sem=doc_recv.at[xp, ens, i],
            device_id={"ens": turn(ens, e, n_ens)}, device_id_type=MESH,
        )

    def doc_arrived(k, i, e):
        xp = turn(x, k, nx)
        ep = turn(ens, e, n_ens)
        piece = emb.at[doc_rows(xp, ep, i), :]
        pltpu.make_async_remote_copy(
            src_ref=piece, dst_ref=piece, send_sem=fwd_send.at[k, 0], recv_sem=doc_recv.at[xp, ep, i],
            device_id={"dp": me}, device_id_type=MESH,
        ).wait_recv()

    def z_copy(c, zo, xo, s):
        place = zo * nx + xo
        return pltpu.make_async_remote_copy(
            src_ref=block(c, zo, xo), dst_ref=block(c, zo, xo),
            send_sem=z_send.at[0 if s > 0 else 1, place], recv_sem=w_recv.at[place, c],
            device_id={"dp": me + s * nx * nc}, device_id_type=MESH,
        )

    def core_copy(c, zo, xo, k):
        return pltpu.make_async_remote_copy(
            src_ref=block(c, zo, xo), dst_ref=block(c, zo, xo),
            send_sem=core_send.at[k], recv_sem=core_recv.at[c, k, jnp.where(zo == far, 1, 0)],
            device_id={"dp": device(z, x, turn(core, k, nc))}, device_id_type=MESH,
        )

    def pass_on(c, zo, xo, sides):
        for s in sides:
            @pl.when((z + s >= 0) & (z + s < nz))
            def _():
                z_copy(c, zo, xo, s).start()
        for k in range(1, nc):
            core_copy(c, zo, xo, k).start()

    def arrived(c, zo, xo):
        pltpu.make_async_remote_copy(
            src_ref=block(c, zo, xo), dst_ref=block(c, zo, xo),
            send_sem=z_send.at[0, 0], recv_sem=w_recv.at[zo * nx + xo, c],
            device_id={"dp": me}, device_id_type=MESH,
        ).wait_recv()

    def from_cores(c, k, is_far):
        blocks = w.at[c, pl.ds(0, (nx if is_far else n_chips - nx) * rows), :]
        return pltpu.make_async_remote_copy(
            src_ref=blocks, dst_ref=blocks, send_sem=core_send.at[k], recv_sem=core_recv.at[c, k, is_far],
            device_id={"dp": device(z, x, turn(core, k, nc))}, device_id_type=MESH,
        )

    for k in range(1, nx):
        loop(chunks, lambda c: x_weights(k, c).start())

    def first(c):
        own_copy(c).wait()
        pass_on(c, z, x, (1, -1))
    loop(chunks, first)
    for k in range(1, nx):
        for i in range(pieces):
            x_docs(k, i).start()
    for copy in (emb_copy, sw_copy, mask_copy, thr_copy):
        copy.start()
    acc[...] = jnp.zeros_like(acc)

    for k in range(1, nx):
        def second(c):
            arrived(c, z, turn(x, k, nx))
            pass_on(c, z, turn(x, k, nx), (1, -1))
        loop(chunks, second)

    def take(d, c):
        for s in (1, -1):
            zo = z + s * d

            @pl.when((zo >= 0) & (zo < nz))
            def _():
                for k in range(nx):
                    arrived(c, zo, turn(x, k, nx))
                    pass_on(c, zo, turn(x, k, nx), (-s,))

    def forward_docs(i):
        for k in range(1, nx):
            doc_arrived(k, i, 0)
            for e in range(1, n_ens):
                doc_forward(k, i, e).start()

    def last_take(c):
        if nz > 1:
            take(nz - 1, c)

    def cores_arrived(c, sides):
        for k in range(1, nc):
            for is_far in sides:
                if is_far or nz > 1:
                    from_cores(c, k, is_far).wait_recv()

    def layer_one(c, row, into):
        hid[row, into] = jnp.maximum(
            jnp.dot(emb[row, :], w[c], preferred_element_type=jnp.float32), 0.0
        ).astype(jnp.bfloat16)

    def member_rows(c, n=1):
        m = c // per_member
        return m, pl.ds(pl.multiple_of(lax.rem(c, per_member) * cols, cols), n * cols)

    def slot_block(k, r):
        return pl.ds(pl.multiple_of(turn(x, k, nx) * docs + r * step_rows, step_rows), step_rows)

    def near_block(at, c, k, r):
        if nz > 1:
            row = slot_block(k, r)
            pre[at, pl.ds(r * step_rows, step_rows), :] = jnp.dot(
                emb[row, near_cols], w[c, near_cols, :], preferred_element_type=jnp.float32
            )
        else:
            pre[at, pl.ds(r * step_rows, step_rows), :] = jnp.zeros((step_rows, cols), jnp.float32)

    def near_own(c):
        cores_arrived(c, (0,))
        for r in range(n_blocks):
            near_block(c, c, 0, r)

    def far_block(at, c, k, r, into):
        row = slot_block(k, r)
        total = pre[at, pl.ds(r * step_rows, step_rows), :] + jnp.dot(
            emb[row, far_cols], w[c, far_cols, :], preferred_element_type=jnp.float32
        )
        hid[row, into] = jnp.maximum(total, 0.0).astype(jnp.bfloat16)

    def layer_two(c, k, into):
        m, at = member_rows(c)
        row = slot(turn(x, k, nx))
        acc[m, row, :] += jnp.dot(hid[row, into], sw[m, at, :], preferred_element_type=jnp.float32)

    def early_slot(k):
        for c in range(early):
            for r in range(n_blocks):
                if k == 0:
                    far_block(c, c, 0, r, pl.ds(c * cols, cols))
                else:
                    layer_one(c, slot_block(k, r), pl.ds(c * cols, cols))
        for c in range(early):
            layer_two(c, k, pl.ds(c * cols, cols))

    def own_chunk(c):
        cores_arrived(c, (1,))
        for r in range(n_blocks):
            far_block(c, c, 0, r, pl.ds(0, cols))
        layer_two(c, 0, pl.ds(0, cols))

    def compute(c):
        @pl.when(jnp.logical_not(inner))
        def _():
            cores_arrived(c, (1,))
            for k in range(nx):
                for r in range(n_blocks):
                    if k == 0:
                        far_block(c, c, 0, r, pl.ds(0, cols))
                    else:
                        layer_one(c, slot_block(k, r), pl.ds(0, cols))
            m, at = member_rows(c)
            acc[m] += jnp.dot(hid[:, 0:cols], sw[m, at, :], preferred_element_type=jnp.float32)

        @pl.when(inner)
        def _():
            for k in range(1, nx):
                for r in range(n_blocks):
                    layer_one(c, slot_block(k, r), pl.ds(0, cols))
                layer_two(c, k, pl.ds(0, cols))

    for copy in (emb_copy, sw_copy, mask_copy, thr_copy):
        copy.wait()
    step_bytes = nx * rows * cols
    share_bytes = (nx - 1) * chunks * rows * cols
    due = {}
    for i in range(pieces):
        at = -(-(share_bytes + (nx - 1) * (i + 1) * doc_piece * width) // step_bytes)
        due.setdefault(min(at, (nz - 2) * chunks - 1), []).append(i)
    for d in range(1, nz - 1):
        def relay(c):
            take(d, c)
            for at, ready in due.items():
                if at // chunks == d - 1:
                    @pl.when(c == at % chunks)
                    def _():
                        for i in ready:
                            forward_docs(i)
            if d == nz - 2:
                @pl.when(c > 0)
                def _():
                    near_own(c - 1)
        loop(chunks, relay)
    if nz < 3:
        loop(final, near_own)
        for i in range(pieces):
            forward_docs(i)
    near_own(final)
    loop(early, last_take)
    for c in range(early):
        cores_arrived(c, (1,))
    early_slot(0)
    last_take(early)

    @pl.when(inner)
    def _():
        loop(chunks - early - 1, lambda i: own_chunk(i + early))
    for k in range(1, nx):
        for e in range(1, n_ens):
            for i in range(pieces):
                doc_arrived(k, i, e)
    for k in range(1, nx):
        early_slot(k)
        for r in range(n_blocks):
            near_block(chunks + k - 1, final, k, r)

    def middle(i):
        last_take(i + early + 1)
        compute(i + early)
    loop(chunks - early - 1, middle)

    cores_arrived(final, (1,))
    final_m, final_at = member_rows(final)

    def piece_of(b):
        return pl.ds(b * piece_rows, piece_rows)

    def mean_part(k, b):
        row = pl.ds(pl.multiple_of(turn(x, k, nx) * docs + b * piece_rows, piece_rows), piece_rows)
        total = acc[0, row, :]
        for m in range(1, members):
            total += acc[m, row, :]
        return total * (1.0 / members)

    def px_copy(k, b):
        return pltpu.make_async_remote_copy(
            src_ref=px_out.at[k, piece_of(b), :], dst_ref=px_in.at[x, piece_of(b), :],
            send_sem=px_send.at[k, b], recv_sem=px_recv.at[x, b],
            device_id={"dp": device(z, turn(x, k, nx), core)}, device_id_type=MESH,
        )

    def send_parts(k, pieces_of_k):
        for b in pieces_of_k:
            px_out[k, piece_of(b), :] = mean_part(k, b).astype(jnp.bfloat16)
            px_copy(k, b).start()

    for k in range(1, nx):
        for r in range(n_blocks):
            far_block(chunks + k - 1, final, k, r, pl.ds(0, cols))
        layer_two(final, k, pl.ds(0, cols))
        send_parts(k, range(AHEAD))

    lines = -(-members // 8) * 8
    wide = members * classes
    lane = lax.broadcasted_iota(jnp.int32, (lines, wide), 1)
    line = lax.broadcasted_iota(jnp.int32, (lines, wide), 0)
    levels = lax.rem(lane, classes).astype(jnp.float32)
    grades = (2.0 * levels / (classes - 1) - 1.0) * jnp.sqrt(jnp.float32(3.0 / classes))
    grades = jnp.where(line == lane // classes, grades, 0.0)
    g_hi = grades.astype(jnp.bfloat16)
    g_lo = (grades - g_hi.astype(jnp.float32)).astype(jnp.bfloat16)
    g = jnp.concatenate([g_hi, g_lo], axis=0)

    def scores_of(xx):
        both = jnp.concatenate([acc[m, slot(xx), :] for m in range(members)], axis=1)
        hi = both.astype(jnp.bfloat16)
        lo = (both - hi.astype(jnp.float32)).astype(jnp.bfloat16)
        dims = (((1,), (1,)), ((), ()))
        s = lax.dot_general(g, hi, dims, preferred_element_type=jnp.float32)
        s += lax.dot_general(g, lo, dims, preferred_element_type=jnp.float32)
        return s[:members] + s[lines : lines + members]

    mine = x * n_ens + ens

    def sc_copy(k, e):
        xp, ep = turn(x, k, nx), turn(ens, e, n_ens)
        return pltpu.make_async_remote_copy(
            src_ref=sc_out.at[k], dst_ref=sc_in.at[mine],
            send_sem=sc_send.at[k, e], recv_sem=sc_recv.at[mine],
            device_id={"dp": device(z, xp, core), "ens": ep}, device_id_type=MESH,
        )

    def sc_arrived(k, e):
        src = turn(x, k, nx) * n_ens + turn(ens, e, n_ens)
        pltpu.make_async_remote_copy(
            src_ref=sc_out.at[k], dst_ref=sc_in.at[src],
            send_sem=sc_send.at[k, e], recv_sem=sc_recv.at[src],
            device_id={"dp": me}, device_id_type=MESH,
        ).wait_recv()

    def send_scores(k):
        s = scores_of(turn(x, k, nx))
        sc_out[k] = s
        if k == 0:
            sc_in[mine] = s
        for e in range(n_ens):
            if k or e:
                sc_copy(k, e).start()

    for k in range(1, nx):
        send_scores(k)
        send_parts(k, range(AHEAD, n_parts))
    for r in range(n_blocks):
        far_block(final, final, 0, r, pl.ds(0, cols))
    acc[final_m, slot(x), :] += jnp.dot(
        hid[slot(x), 0:cols], sw[final_m, final_at, :], preferred_element_type=jnp.float32
    )
    send_scores(0)

    def px_arrived(k, b):
        xp = turn(x, k, nx)
        pltpu.make_async_remote_copy(
            src_ref=px_in.at[xp, piece_of(b), :], dst_ref=px_in.at[xp, piece_of(b), :],
            send_sem=px_send.at[k, b], recv_sem=px_recv.at[xp, b],
            device_id={"dp": me}, device_id_type=MESH,
        ).wait_recv()

    def part_copy(e, b):
        piece = part.at[ens, piece_of(b), :]
        return pltpu.make_async_remote_copy(
            src_ref=piece, dst_ref=piece, send_sem=part_send.at[e, b], recv_sem=part_recv.at[ens, b],
            device_id={"ens": turn(ens, e, n_ens)}, device_id_type=MESH,
        )

    def relay_part(b):
        total = mean_part(0, b)
        for k in range(1, nx):
            px_arrived(k, b)
            total += px_in[turn(x, k, nx), piece_of(b), :].astype(jnp.float32)
        part[ens, piece_of(b), :] = total.astype(jnp.bfloat16)
        for e in range(1, n_ens):
            part_copy(e, b).start()

    for k in range(1, nx):
        whole = w.at[:, origin_rows(me), :]
        pltpu.make_async_remote_copy(
            src_ref=whole, dst_ref=whole, send_sem=x_send.at[k], recv_sem=w_recv.at[0, 0],
            device_id={"dp": device(z, turn(x, k, nx), core)}, device_id_type=MESH,
        ).wait_send()
        docs_out = emb.at[pl.ds(0, doc_part), :]
        pltpu.make_async_remote_copy(
            src_ref=docs_out, dst_ref=docs_out, send_sem=doc_send.at[k], recv_sem=doc_recv.at[0, 0, 0],
            device_id={"dp": device(z, turn(x, k, nx), core)}, device_id_type=MESH,
        ).wait_send()
        for e in range(1, n_ens):
            pltpu.make_async_remote_copy(
                src_ref=docs_out, dst_ref=docs_out, send_sem=fwd_send.at[k, e], recv_sem=doc_recv.at[0, 0, 0],
                device_id={"ens": turn(ens, e, n_ens)}, device_id_type=MESH,
            ).wait_send()
    for place in range(n_chips):
        zo, xo = divmod(place, nx)
        for s in (1, -1):
            @pl.when((z + s >= 0) & (z + s < nz) & ((zo <= z) if s > 0 else (zo >= z)))
            def _():
                whole = w.at[:, origin_rows(device(zo, xo, core)), :]
                pltpu.make_async_remote_copy(
                    src_ref=whole, dst_ref=whole,
                    send_sem=z_send.at[0 if s > 0 else 1, place], recv_sem=w_recv.at[0, 0],
                    device_id={"dp": me + s * nx * nc}, device_id_type=MESH,
                ).wait_send()
    for k in range(1, nc):
        blocks = w.at[:, pl.ds(0, n_chips * rows), :]
        pltpu.make_async_remote_copy(
            src_ref=blocks, dst_ref=blocks, send_sem=core_send.at[k], recv_sem=core_recv.at[0, k, 0],
            device_id={"dp": device(z, x, turn(core, k, nc))}, device_id_type=MESH,
        ).wait_send()
    relay_part(0)
    for k, e in others:
        sc_arrived(k, e)
    scores = sc_in[0]
    for k in range(1, nx * n_ens):
        scores += sc_in[k]
    row = lax.broadcasted_iota(jnp.int32, (members, docs), 0)
    cutoff = jnp.zeros((members, docs), jnp.float32)
    mean_cutoff = jnp.float32(0.0)
    for m in range(members):
        level = thr[m].astype(jnp.float32) * (1.0 / 256.0)
        cutoff = jnp.where(row == m, level, cutoff)
        mean_cutoff += level * (1.0 / members)
    kept = mask[...].reshape(1, docs).astype(jnp.float32) * jax.nn.sigmoid(4.0 * (scores - cutoff))
    ens_score = jnp.sum(scores, axis=0, keepdims=True) * (1.0 / members)
    ens_kept = jax.nn.sigmoid(4.0 * (ens_score - mean_cutoff))
    kept_sum = jnp.sum(kept, axis=1, keepdims=True)
    agree_sum = jnp.sum(kept * ens_kept, axis=1, keepdims=True)
    lane = lax.broadcasted_iota(jnp.int32, (members, 128), 1)
    line = lax.broadcasted_iota(jnp.int32, (members, 128), 0)
    own = members // n_ens
    mine_at = line - ens * own
    is_mine = (mine_at >= 0) & (mine_at < own)
    spread = jnp.where(is_mine & (lane == mine_at), kept_sum, 0.0)
    spread += jnp.where(is_mine & (lane == mine_at + own), agree_sum, 0.0)
    tot[me] = jnp.sum(spread, axis=0, keepdims=True)

    def tot_copy(k):
        return pltpu.make_async_remote_copy(
            src_ref=tot.at[me], dst_ref=tot.at[me], send_sem=tot_sem.at[0], recv_sem=tot_sem.at[1],
            device_id={"dp": lax.rem(me + k, n_dp)}, device_id_type=MESH,
        )

    tiles = tot.at[pl.ds(0, n_dp - 1)]
    all_tot = pltpu.make_async_remote_copy(
        src_ref=tiles, dst_ref=tiles, send_sem=tot_sem.at[0], recv_sem=tot_sem.at[1],
        device_id={"dp": lax.rem(me + 1, n_dp)}, device_id_type=MESH,
    )
    for k in range(1, n_dp):
        tot_copy(k).start()

    for b in range(1, n_parts):
        relay_part(b)

    for b in range(n_parts):
        for e in range(1, n_ens):
            other = turn(ens, e, n_ens)
            block_in = part.at[other, piece_of(b), :]
            pltpu.make_async_remote_copy(
                src_ref=block_in, dst_ref=block_in, send_sem=part_send.at[e, b], recv_sem=part_recv.at[other, b],
                device_id={"ens": other}, device_id_type=MESH,
            ).wait_recv()
        total = part[0, piece_of(b), :].astype(jnp.float32)
        for e in range(1, n_ens):
            total += part[e, piece_of(b), :].astype(jnp.float32)
        out_ref[piece_of(b), :] = total

    all_tot.wait_recv()
    sums = tot[0]
    for k in range(1, n_dp):
        sums += tot[k]
    share_ref[...] = sums / docs

    for k, e in others:
        sc_copy(k, e).wait_send()
    for b in range(n_parts):
        for k in range(1, nx):
            px_copy(k, b).wait_send()
        for e in range(1, n_ens):
            part_copy(e, b).wait_send()
    all_tot.wait_send()


def solution(mesh):
    geo = geometry(mesh)
    nz, nx, nc = geo
    n_dp, n_ens = mesh.shape["dp"], mesh.shape["ens"]

    def on_device(embeddings, valid_mask, first_weight, second_weight, thresholds):
        docs, width = embeddings.shape
        members, rows, units = first_weight.shape
        classes = second_weight.shape[2]
        share = units // nx
        cols = min(COLS, share)
        chunks = members * share // cols
        own = members // n_ens
        early = min(EARLY, chunks - 1)
        parts = docs // math.gcd(docs, ROWS) * SPLIT
        pieces = math.gcd(docs // n_ens // 16, PIECES)
        dma = pltpu.SemaphoreType.DMA
        hbm, vmem = (pl.BlockSpec(memory_space=s) for s in (pl.ANY, pltpu.VMEM))
        mean_logits, shares = pl.pallas_call(
            functools.partial(kernel, geo, n_ens),
            out_shape=(
                pltpu.VMEM((docs, classes), jnp.float32),
                pltpu.VMEM((1, 128), jnp.float32),
            ),
            in_specs=[hbm] * 5,
            out_specs=(vmem, vmem),
            scratch_shapes=[
                pltpu.VMEM((chunks, width, cols), jnp.bfloat16),
                pltpu.VMEM((nx * docs, width), jnp.bfloat16),
                pltpu.VMEM((members, share, classes), jnp.bfloat16),
                pltpu.VMEM((members, nx * docs, classes), jnp.float32),
                pltpu.VMEM((nx * docs, early * cols), jnp.bfloat16),
                pltpu.VMEM((chunks + nx - 1, docs, cols), jnp.float32),
                pltpu.VMEM(valid_mask.shape, valid_mask.dtype),
                pltpu.SMEM(thresholds.shape, thresholds.dtype),
                pltpu.VMEM((nx, docs, classes), jnp.bfloat16),
                pltpu.VMEM((nx, docs, classes), jnp.bfloat16),
                pltpu.VMEM((n_ens, docs, classes), jnp.bfloat16),
                pltpu.VMEM((nx, members, docs), jnp.float32),
                pltpu.VMEM((nx * n_ens, members, docs), jnp.float32),
                pltpu.VMEM((n_dp, 1, 128), jnp.float32),
                dma((chunks,)),
                dma((4,)),
                dma((2, nz * nx)),
                dma((nz * nx, chunks)),
                dma((nx,)),
                dma((nc,)),
                dma((chunks, nc, 2)),
                dma((nx,)),
                dma((nx, n_ens, pieces)),
                dma((nx, n_ens)),
                dma((nx, parts)),
                dma((nx, parts)),
                dma((n_ens, parts)),
                dma((n_ens, parts)),
                dma((nx, n_ens)),
                dma((nx * n_ens,)),
                dma((2,)),
            ],
            compiler_params=pltpu.CompilerParams(
                collective_id=0, has_side_effects=True, vmem_limit_bytes=63 * 1024 * 1024
            ),
        )(embeddings, valid_mask, first_weight, second_weight, thresholds)
        return mean_logits, shares[0, :own], shares[0, own : 2 * own]

    return jax.shard_map(
        on_device,
        mesh=mesh,
        in_specs=(P("dp", None), P("dp"), P(None, "dp", "ens"), P(None, "ens", None), P()),
        out_specs=(P("dp", None), P("ens"), P("ens")),
        check_vma=False,
    )
```
